32 devices in a mesh: seq: 8 (over y, x, core), head: 4 (over z).
Axes of the slice: x: 2, y: 2, z: 4, core: 2. Of those that a mesh axis runs over, the one named last changes fastest.
Arguments:
- mid: bfloat16 [2048, 3072], P('seq'), may hold values from -20 to 20
- second_in: bfloat16 [2048, 3072], P('seq'), may hold values from -20 to 20
- cotangent: bfloat16 [2048, 3072], P('seq'), may hold values from -6 to 6
- w_key: bfloat16 [3072, 1024], P(None, 'head'), may hold values from -0.109375 to 0.109375
- w_value: bfloat16 [3072, 1024], P(None, 'head'), may hold values from -0.109375 to 0.109375
- w_query: bfloat16 [2, 3072, 3072], P(None, None, 'head'), may hold values from -0.109375 to 0.109375
- w_out: bfloat16 [2, 3072, 3072], P(None, 'head'), may hold values from -0.109375 to 0.109375
- w_ret_out: bfloat16 [3072, 3072], P('head'), may hold values from -0.109375 to 0.109375
- ret_query: bfloat16 [2048, 3072], P('seq', 'head'), may hold values from -6 to 6
- ret_key: bfloat16 [2048, 3072], P('seq', 'head'), may hold values from -3 to 3
- ret_value: bfloat16 [2048, 3072], P('seq', 'head'), may hold values from -6 to 6
- gate: float32 [24, 2048], P('head', 'seq'), may hold values from 0 to 6
- decay_exp: int32 [24], P('head'), may hold values from 0 to 256
- mask_start: int32 [16], P('seq'), may hold values from 0 to 1920, as said below
Outputs:
- grad_mid: bfloat16 [2048, 3072], P('seq')
- grad_ret_query: bfloat16 [2048, 3072], P('seq', 'head')
- grad_ret_key: bfloat16 [2048, 3072], P('seq', 'head')
- grad_ret_value: bfloat16 [2048, 3072], P('seq', 'head')
- grad_w_key: float32 [3072, 1024], P(None, 'head')
- grad_w_value: float32 [3072, 1024], P(None, 'head')
The draws below stay inside these ranges and needn't reach their ends.
Inputs may be any that keep to these rules, and one draw needn't show every extreme that they name: `mask_start`: the entry of each block of 128 queries is at most the position of that block's first query.
All inputs are finite; a program needn't handle non-finite values.
Results may differ from the reference program's by a relative error of at most 0.025.
The reference program's roundings to bfloat16 on the way count: a program that leaves them out, or rounds other values in their place, can miss the bound.
Values may be sent and summed in bfloat16 or wider, within the bound.
A program may use at most 192 MiB of HBM per device.

```python
import math
import jax
import jax.numpy as jnp
from jax import lax

D = 3072
H = 24
KVH = 8
HR = 24
E = 128
LAYERS = 2
BLK = 128
RC = 128
TOK_DEV = 256
TOKENS = 2048


def rows_with_peaks(key):
    values = jnp.clip(jax.random.normal(key, (TOKENS, D), jnp.float32), -5.0, 5.0)
    return values.astype(jnp.bfloat16)


def draw_mid(key, part):
    return rows_with_peaks(key)


def draw_second_in(key, part):
    return rows_with_peaks(jax.random.fold_in(key, 11))


def draw_gate(key, part):
    chooser, rough_key, block_key = jax.random.split(key, 3)
    portion = 0.5
    lasting = jax.random.uniform(chooser, (HR, 1), jnp.float32) < portion
    rough = jax.random.uniform(rough_key, (HR, TOKENS), jnp.float32, 0.5, 2.0)
    blocks = jax.random.uniform(block_key, (HR, TOKENS // TOK_DEV), jnp.float32, 0.5, 2.0)
    rough = rough * jnp.repeat(blocks, TOK_DEV, axis=1)
    factor = jnp.where(lasting, 0.5 / TOKENS, 1.5)
    return (factor * rough).astype(jnp.float32)


def draw_mask_start(key, part):
    blocks = TOKENS // BLK
    firsts = jnp.arange(blocks, dtype=jnp.int32) * BLK
    drawn = jax.random.randint(key, (blocks,), 0, firsts + 1, dtype=jnp.int32)
    last_block = jnp.arange(blocks, dtype=jnp.int32) == blocks - 1
    return jnp.where(last_block, firsts, drawn).astype(jnp.int32)


def with_ends(result, stream_key, least, top_value):
    longest = result.shape.index(max(result.shape))
    spots = []
    for shift in (0, 1):
        where = [jax.random.randint(jax.random.fold_in(stream_key, axis), (), 0, length) for axis, length in enumerate(result.shape)]
        where[longest] = (where[longest] + shift) % result.shape[longest]
        spots.append(tuple(where))
    return result.at[spots[0]].set(least).at[spots[1]].set(top_value)


def steps_of(rng, dims, cuts, smallest, high):
    loudness = 1.0
    for position, parts in cuts:
        steps = jax.random.uniform(jax.random.fold_in(jax.random.fold_in(rng, 6), position), (parts,), jnp.float32, smallest / len(cuts), high / len(cuts))
        loudness = loudness * jnp.repeat(jnp.exp(steps), dims[position] // parts).reshape((-1,) + (1,) * (len(dims) - 1 - position))
    return loudness


def gaussian(rng, shape, spread, bound, shards=(), kind=jnp.bfloat16):
    factor_of = steps_of(rng, shape, shards, -0.22, 0.18) if shards else 1.0
    result = jax.random.normal(rng, shape, jnp.float32) * spread * factor_of
    return jnp.minimum(jnp.maximum(result, -bound), bound).astype(kind)


def setup_inputs(seed: int = 0) -> dict:
    streams_of = jax.random.split(jax.random.key(seed), 15)
    return {
        "mid": draw_mid(jax.random.fold_in(streams_of[14], 71), 0),
        "second_in": draw_second_in(jax.random.fold_in(streams_of[14], 71), 0),
        "cotangent": gaussian(streams_of[2], (TOKENS, D), 1.0, 6.0, ((0, 8),)),
        "w_key": gaussian(streams_of[3], (D, KVH * E), D ** -0.5, 0.109375, ((1, 4),)),
        "w_value": gaussian(streams_of[4], (D, KVH * E), D ** -0.5, 0.109375, ((1, 4),)),
        "w_query": gaussian(streams_of[5], (LAYERS, D, H * E), D ** -0.5, 0.109375, ((2, 4),)),
        "w_out": gaussian(streams_of[6], (LAYERS, H * E, D), (H * E) ** -0.5, 0.109375, ((1, 4),)),
        "w_ret_out": gaussian(streams_of[7], (HR * E, D), (HR * E) ** -0.5, 0.109375, ((0, 4),)),
        "ret_query": gaussian(streams_of[8], (TOKENS, HR * E), 1.0, 6.0, ((0, 8), (1, 4))),
        "ret_key": gaussian(streams_of[9], (TOKENS, HR * E), 0.5, 3.0, ((0, 8), (1, 4))),
        "ret_value": gaussian(streams_of[10], (TOKENS, HR * E), 1.0, 6.0, ((0, 8), (1, 4))),
        "gate": draw_gate(jax.random.fold_in(streams_of[14], 71), 0),
        "decay_exp": with_ends(jax.random.randint(streams_of[12], (HR,), 0, 257), jax.random.fold_in(streams_of[12], 1), 0, 256).astype(jnp.int32),
        "mask_start": draw_mask_start(jax.random.fold_in(streams_of[14], 71), 0),
    }


def contract_last(left, right):
    return lax.dot_general(left, right, (((1,), (1,)), ((), ())), preferred_element_type=jnp.float32)

def round_trip(value):
    return lax.optimization_barrier(value.astype(jnp.bfloat16)).astype(jnp.float32)

def attend_back(layer_in, w_query_l, w_out_l, upstream, keys, values, visible):
    length = layer_in.shape[0]
    kv_heads = keys.shape[1] // E
    factor = 1.0 / math.sqrt(E)
    queries = jnp.dot(layer_in, w_query_l, preferred_element_type=jnp.float32).astype(jnp.bfloat16)
    group = queries.shape[1] // keys.shape[1]
    grad_out = contract_last(upstream, w_out_l).astype(jnp.bfloat16)
    query_heads = queries.reshape(length, kv_heads, group, E).transpose(1, 2, 0, 3)
    grad_heads = grad_out.reshape(length, kv_heads, group, E).transpose(1, 2, 0, 3)
    key_heads = keys.reshape(length, kv_heads, E).transpose(1, 0, 2)
    value_heads = values.reshape(length, kv_heads, E).transpose(1, 0, 2)

    def one_group(items):
        query_now = items[0].astype(jnp.float32)
        grad_now = items[1].astype(jnp.float32)
        key_now = items[2].astype(jnp.float32)
        value_now = items[3].astype(jnp.float32)
        scores = jnp.einsum('gte,se->gts', query_now, key_now) * factor
        scores = jnp.where(visible, scores, -jnp.inf)
        top = lax.optimization_barrier(jnp.max(scores, axis=-1, keepdims=True))
        raised = jnp.exp(scores - top)
        probs = raised / lax.optimization_barrier(jnp.sum(raised, axis=-1, keepdims=True))
        rounded = round_trip(probs)
        outputs = round_trip(jnp.einsum('gts,se->gte', rounded, value_now))
        delta = lax.optimization_barrier(jnp.sum(grad_now * outputs, axis=-1, keepdims=True))
        dprobs = jnp.einsum('gte,se->gts', grad_now, value_now)
        dscores = round_trip(probs * (dprobs - delta) * factor)
        query_grad = jnp.einsum('gts,se->gte', dscores, key_now).astype(jnp.bfloat16)
        key_part = jnp.einsum('gts,gte->se', dscores, query_now)
        value_part = jnp.einsum('gts,gte->se', rounded, grad_now)
        return (query_grad, key_part, value_part)
    query_grads, key_parts, value_parts = lax.map(one_group, (query_heads, grad_heads, key_heads, value_heads))
    query_grad = query_grads.transpose(2, 0, 1, 3).reshape(length, -1)
    key_part = key_parts.transpose(1, 0, 2).reshape(length, -1)
    value_part = value_parts.transpose(1, 0, 2).reshape(length, -1)
    return (contract_last(query_grad, w_query_l), key_part, value_part)

def retention_states(ret_key, ret_value, gate, decay_exp):
    length, width = ret_key.shape
    heads = gate.shape[0]
    size = width // heads
    count = length // RC
    key_blocks = ret_key.reshape(count, RC, heads, size).astype(jnp.float32)
    value_blocks = ret_value.reshape(count, RC, heads, size).astype(jnp.float32)
    rate = jnp.exp2(-decay_exp.astype(jnp.float32) / 64.0)
    accum = jnp.cumsum((-rate[:, None] * gate).reshape(heads, count, RC), axis=2)
    ends = accum[:, :, -1]
    shrink = jnp.transpose(jnp.exp(ends[:, :, None] - accum), (1, 2, 0))[..., None]
    own_state = jnp.einsum('csha,cshb->hcab', round_trip(shrink * key_blocks), value_blocks)
    return (accum, ends, shrink, own_state)

def grad_states(ret_query, grad_o, accum):
    heads, count, block = accum.shape
    size = ret_query.shape[1] // heads
    query_blocks = ret_query.reshape(count, block, heads, size).astype(jnp.float32)
    grad_blocks = grad_o.reshape(count, block, heads, size).astype(jnp.float32)
    grow = jnp.transpose(jnp.exp(accum), (1, 2, 0))[..., None]
    own_grad = jnp.einsum('ctha,cthb->hcab', round_trip(grow * query_blocks), grad_blocks) / E
    return (grow, own_grad)

def retention_grads(ret_query, ret_key, ret_value, grad_o, accum, shrink, grow, entering, after):
    length, width = ret_query.shape
    heads, count, block = accum.shape
    size = width // heads
    shape4 = (count, block, heads, size)
    query_blocks = ret_query.reshape(shape4).astype(jnp.float32)
    key_blocks = ret_key.reshape(shape4).astype(jnp.float32)
    value_blocks = ret_value.reshape(shape4).astype(jnp.float32)
    grad_blocks = grad_o.reshape(shape4).astype(jnp.float32)
    lower = jnp.arange(block)[:, None] >= jnp.arange(block)[None, :]
    diff = accum[:, :, :, None] - accum[:, :, None, :]
    weights = jnp.where(lower, jnp.exp(jnp.where(lower, diff, 0.0)), 0.0)
    first = round_trip(weights * jnp.einsum('ctha,csha->hcts', grad_blocks, value_blocks))
    second = round_trip(weights * jnp.einsum('ctha,csha->hcts', query_blocks, key_blocks))
    inner_query = jnp.einsum('hcts,csha->ctha', first, key_blocks)
    inner_key = jnp.einsum('hcts,ctha->csha', first, query_blocks)
    inner_value = jnp.einsum('hcts,ctha->csha', second, grad_blocks)
    highest = lax.Precision.HIGHEST
    carried_query = jnp.einsum('cthb,hcab->ctha', grad_blocks, entering, precision=highest)
    carried_key = jnp.einsum('cshb,hcab->csha', value_blocks, after, precision=highest)
    carried_value = jnp.einsum('csha,hcab->cshb', key_blocks, after, precision=highest)
    grad_query = ((inner_query + grow * carried_query) / E).astype(jnp.bfloat16).reshape(length, width)
    grad_key = (inner_key / E + shrink * carried_key).astype(jnp.bfloat16).reshape(length, width)
    grad_value = (inner_value / E + shrink * carried_value).astype(jnp.bfloat16).reshape(length, width)
    return (grad_query, grad_key, grad_value)

def reference(mid, second_in, cotangent, w_key, w_value, w_query, w_out, w_ret_out, ret_query, ret_key, ret_value, gate, decay_exp, mask_start):
    keys = jnp.dot(mid, w_key, preferred_element_type=jnp.float32).astype(jnp.bfloat16)
    values = jnp.dot(mid, w_value, preferred_element_type=jnp.float32).astype(jnp.bfloat16)
    positions = jnp.arange(TOKENS, dtype=jnp.int32)
    first_seen = jnp.repeat(mask_start, BLK)
    visible = (positions[None, :] >= first_seen[:, None]) & (positions[None, :] <= positions[:, None])
    upper_in, upper_key, upper_value = attend_back(second_in, w_query[1], w_out[1], cotangent, keys, values, visible)
    upstream = (cotangent.astype(jnp.float32) + upper_in).astype(jnp.bfloat16)
    lower_in, lower_key, lower_value = attend_back(mid, w_query[0], w_out[0], upstream, keys, values, visible)
    key_grad = (upper_key + lower_key).astype(jnp.bfloat16)
    value_grad = (upper_value + lower_value).astype(jnp.bfloat16)
    grad_mid = (upstream.astype(jnp.float32) + lower_in + contract_last(key_grad, w_key) + contract_last(value_grad, w_value)).astype(jnp.bfloat16)
    tokens_dims = (((0,), (0,)), ((), ()))
    grad_w_key = lax.dot_general(mid, key_grad, tokens_dims, preferred_element_type=jnp.float32)
    grad_w_value = lax.dot_general(mid, value_grad, tokens_dims, preferred_element_type=jnp.float32)
    grad_o = contract_last(grad_mid, w_ret_out).astype(jnp.bfloat16)
    accum, ends, shrink, own_state = retention_states(ret_key, ret_value, gate, decay_exp)
    grow, own_grad = grad_states(ret_query, grad_o, accum)
    decays = jnp.exp(ends)
    zeros = jnp.zeros((gate.shape[0], E, E), jnp.float32)

    def forward(state, items):
        return (items[0][:, None, None] * state + items[1], state)

    def backward(state, items):
        return (items[1] + items[0][:, None, None] * state, state)
    unused_state, entering = lax.scan(forward, zeros, (decays.T, jnp.moveaxis(own_state, 1, 0)))
    unused_grad, after = lax.scan(backward, zeros, (decays.T, jnp.moveaxis(own_grad, 1, 0)), reverse=True)
    entering = jnp.moveaxis(entering, 0, 1)
    after = jnp.moveaxis(after, 0, 1)
    grad_query, grad_key, grad_value = retention_grads(ret_query, ret_key, ret_value, grad_o, accum, shrink, grow, entering, after)
    return (grad_mid, grad_query, grad_key, grad_value, grad_w_key, grad_w_value)
```

```python
import functools
import math

import jax
import jax.numpy as jnp
from jax import lax
from jax.experimental import pallas as pl
from jax.experimental.pallas import tpu as pltpu
from jax.sharding import PartitionSpec as P

E = 128
BLK = 128
RC = 128
F32 = jnp.float32
BF16 = jnp.bfloat16


def contract_last(left, right):
    return lax.dot_general(left, right, (((1,), (1,)), ((), ())), preferred_element_type=F32)


def contract_first(left, right):
    return lax.dot_general(left, right, (((0,), (0,)), ((), ())), preferred_element_type=F32)


def attention_kernel(group, step, has_prev, mask_ref, *refs):
    if has_prev:
        q_ref, g_ref, k_ref, v_ref, pk_ref, pv_ref, dq_ref, dk_ref, dv_ref = refs[:9]
        s_ref, dk_acc, dv_acc = refs[9:]
    else:
        q_ref, g_ref, k_ref, v_ref, dq_ref, dk_ref, dv_ref, s_ref = refs
        dk_acc, dv_acc = dk_ref, dv_ref
    factor = 1.0 / math.sqrt(E)
    block = pl.program_id(1)
    first_row = mask_ref[0] + block * BLK
    first_key = mask_ref[1 + block]
    rows = group * BLK

    @pl.when(block == 0)
    def _():
        if has_prev:
            dk_acc[...] = pk_ref[...]
            dv_acc[...] = pv_ref[...]
        else:
            dk_acc[...] = jnp.zeros_like(dk_acc)
            dv_acc[...] = jnp.zeros_like(dv_acc)

    q = jnp.concatenate([q_ref[:, i * E : (i + 1) * E] for i in range(group)], axis=0)
    g = jnp.concatenate([g_ref[:, i * E : (i + 1) * E] for i in range(group)], axis=0)
    low = first_key // step
    high = (first_row + BLK + step - 1) // step
    query_position = first_row + lax.broadcasted_iota(jnp.int32, (BLK, step), 0)

    def span(j):
        return pl.ds(pl.multiple_of(j * step, step), step)

    def score(j, top):
        scores = contract_last(q, k_ref[span(j), :]) * factor
        at = j * step + lax.broadcasted_iota(jnp.int32, (BLK, step), 1)
        seen = (at >= first_key) & (at <= query_position)
        seen = jnp.concatenate([seen] * group, axis=0)
        scores = jnp.where(seen, scores, -jnp.inf)
        s_ref[:, span(j)] = scores
        return jnp.maximum(top, jnp.max(scores, axis=-1, keepdims=True))

    top = lax.fori_loop(low, high, score, jnp.full((rows, 1), -jnp.inf, F32))

    def raise_(j, total):
        raised = jnp.exp(s_ref[:, span(j)] - top)
        s_ref[:, span(j)] = raised
        return total + jnp.sum(raised, axis=-1, keepdims=True)

    total = lax.fori_loop(low, high, raise_, jnp.zeros((rows, 1), F32))
    scale = 1.0 / total

    def output(j, out):
        probs = s_ref[:, span(j)] * scale
        s_ref[:, span(j)] = probs
        return out + jnp.dot(probs.astype(BF16), v_ref[span(j), :], preferred_element_type=F32)

    out = lax.fori_loop(low, high, output, jnp.zeros((rows, E), F32)).astype(BF16)
    delta = jnp.sum(g.astype(F32) * out.astype(F32), axis=-1, keepdims=True)

    def back(j, dq):
        probs = s_ref[:, span(j)]
        dprobs = contract_last(g, v_ref[span(j), :])
        dscores = (probs * (dprobs - delta) * factor).astype(BF16)
        dk_acc[span(j), :] += contract_first(dscores, q)
        dv_acc[span(j), :] += contract_first(probs.astype(BF16), g)
        return dq + jnp.dot(dscores, k_ref[span(j), :], preferred_element_type=F32)

    dq = lax.fori_loop(low, high, back, jnp.zeros((rows, E), F32)).astype(BF16)
    for i in range(group):
        dq_ref[:, i * E : (i + 1) * E] = dq[i * BLK : (i + 1) * BLK, :]
    if has_prev:

        @pl.when(block == pl.num_programs(1) - 1)
        def _():
            dk_ref[...] = dk_acc[...].astype(BF16)
            dv_ref[...] = dv_acc[...].astype(BF16)


def attention(mask, queries, grad_out, kv, previous):
    row_count, width = queries.shape
    key_count, both = kv.shape
    heads = both // (2 * E)
    group = width // (heads * E)
    step = 256 if key_count % 256 == 0 else BLK
    has_prev = previous is not None
    tile = pl.BlockSpec((BLK, group * E), lambda h, b, m: (b, h))
    key_block = pl.BlockSpec((key_count, E), lambda h, b, m: (0, h))
    value_block = pl.BlockSpec((key_count, E), lambda h, b, m: (0, h + heads))
    part = jax.ShapeDtypeStruct((key_count, heads * E), BF16 if has_prev else F32)
    scratch = [pltpu.VMEM((group * BLK, key_count), F32)]
    if has_prev:
        scratch += [pltpu.VMEM((key_count, E), F32)] * 2
    return pl.pallas_call(
        functools.partial(attention_kernel, group, step, has_prev),
        out_shape=(jax.ShapeDtypeStruct((row_count, width), BF16), part, part),
        grid_spec=pltpu.PrefetchScalarGridSpec(
            num_scalar_prefetch=1,
            grid=(heads, row_count // BLK),
            in_specs=[tile, tile, key_block, value_block] + [key_block] * (2 if has_prev else 0),
            out_specs=(tile, key_block, key_block),
            scratch_shapes=scratch,
        ),
        compiler_params=pltpu.CompilerParams(vmem_limit_bytes=48 * 2**20),
        cost_estimate=pl.CostEstimate(
            flops=10 * row_count * width * key_count, bytes_accessed=8 * 2**20, transcendentals=0
        ),
        name="attention_back",
    )(mask, queries, grad_out, kv, kv, *(previous or ()))


def retention_states(ret_key, ret_value, gate, decay_exp):
    length, width = ret_key.shape
    heads = gate.shape[0]
    size = width // heads
    count = length // RC
    key_blocks = ret_key.reshape(count, RC, heads, size)
    value_blocks = ret_value.reshape(count, RC, heads, size)
    rate = jnp.exp2(-decay_exp.astype(F32) / 64.0)
    accum = jnp.cumsum((-rate[:, None] * gate).reshape(heads, count, RC), axis=2)
    ends = accum[:, :, -1]
    shrink = jnp.transpose(jnp.exp(ends[:, :, None] - accum), (1, 2, 0))[..., None]
    weighted = (shrink * key_blocks).astype(BF16)
    own_state = jnp.einsum("csha,cshb->hcab", weighted, value_blocks, preferred_element_type=F32)
    return (accum, ends, shrink, own_state)


def grad_states(ret_query, grad_o, accum):
    heads, count, block = accum.shape
    size = ret_query.shape[1] // heads
    query_blocks = ret_query.reshape(count, block, heads, size)
    grad_blocks = grad_o.reshape(count, block, heads, size)
    grow = jnp.transpose(jnp.exp(accum), (1, 2, 0))[..., None]
    weighted = (grow * query_blocks).astype(BF16)
    own_grad = jnp.einsum("ctha,cthb->hcab", weighted, grad_blocks, preferred_element_type=F32) / E
    return (grow, own_grad)


def retention_grads(ret_query, ret_key, ret_value, grad_o, accum, shrink, grow, entering, after):
    length, width = ret_query.shape
    heads, count, block = accum.shape
    size = width // heads
    shape4 = (count, block, heads, size)
    query_blocks = ret_query.reshape(shape4)
    key_blocks = ret_key.reshape(shape4)
    value_blocks = ret_value.reshape(shape4)
    grad_blocks = grad_o.reshape(shape4)
    lower = jnp.arange(block)[:, None] >= jnp.arange(block)[None, :]
    diff = accum[:, :, :, None] - accum[:, :, None, :]
    weights = jnp.where(lower, jnp.exp(jnp.where(lower, diff, 0.0)), 0.0)
    dot = functools.partial(jnp.einsum, preferred_element_type=F32)
    first = (weights * dot("ctha,csha->hcts", grad_blocks, value_blocks)).astype(BF16)
    second = (weights * dot("ctha,csha->hcts", query_blocks, key_blocks)).astype(BF16)
    inner_query = dot("hcts,csha->ctha", first, key_blocks)
    inner_key = dot("hcts,ctha->csha", first, query_blocks)
    inner_value = dot("hcts,ctha->csha", second, grad_blocks)
    entering = entering.astype(BF16)
    after = after.astype(BF16)
    carried_query = dot("cthb,hcab->ctha", grad_blocks, entering)
    carried_key = dot("cshb,hcab->csha", value_blocks, after)
    carried_value = dot("csha,hcab->cshb", key_blocks, after)
    grad_query = ((inner_query + grow * carried_query) / E).astype(BF16).reshape(length, width)
    grad_key = (inner_key / E + shrink * carried_key).astype(BF16).reshape(length, width)
    grad_value = (inner_value / E + shrink * carried_value).astype(BF16).reshape(length, width)
    return (grad_query, grad_key, grad_value)


def head_total(partial_value, residual):
    summed = lax.psum(partial_value.astype(BF16), "head")
    return (residual.astype(F32) + summed.astype(F32)).astype(BF16)


def gather_states(state):
    heads = state.shape[0]
    return lax.all_gather(state.astype(BF16).reshape(heads * E, E), "seq")


def local(
    mid,
    second_in,
    cotangent,
    w_key,
    w_value,
    w_query,
    w_out,
    w_ret_out,
    ret_query,
    ret_key,
    ret_value,
    gate,
    decay_exp,
    mask_start,
):
    row_count = mid.shape[0]
    peers, position = lax.axis_size("seq"), lax.axis_index("seq")
    accum, ends, shrink, own_state = retention_states(ret_key, ret_value, gate, decay_exp)
    decay_rows = jnp.exp(ends)
    heads, count = decay_rows.shape
    device_decay = jnp.prod(decay_rows, axis=1)
    device_state = jnp.zeros_like(own_state[:, 0])
    for block in range(count):
        device_state = decay_rows[:, block, None, None] * device_state + own_state[:, block]
    states = gather_states(device_state).reshape(peers, heads, E, E)
    decays = lax.all_gather(jnp.broadcast_to(device_decay[:, None], (heads, E)), "seq")[:, :, 0]
    forward, backward = [], []
    for k in range(peers):
        pf = jnp.where(k < position, 1.0, 0.0) * jnp.ones((heads,), F32)
        pb = jnp.where(k > position, 1.0, 0.0) * jnp.ones((heads,), F32)
        for m in range(peers):
            if m > k:
                pf = pf * jnp.where(m < position, decays[m], 1.0)
            if m < k:
                pb = pb * jnp.where(m > position, decays[m], 1.0)
        forward.append(pf)
        backward.append(pb)
    incoming = sum(c[:, None, None] * states[k].astype(F32) for k, c in enumerate(forward))

    kv_own = jnp.concatenate(
        [
            jnp.dot(mid, w_key, preferred_element_type=F32).astype(BF16),
            jnp.dot(mid, w_value, preferred_element_type=F32).astype(BF16),
        ],
        axis=1,
    )
    kv = lax.all_gather(kv_own, "seq", axis=0, tiled=True)
    mask = jnp.concatenate([(position * row_count)[None].astype(jnp.int32), mask_start])
    width = w_key.shape[1]

    queries = jnp.dot(second_in, w_query[1], preferred_element_type=F32).astype(BF16)
    grad_out = contract_last(cotangent, w_out[1]).astype(BF16)
    query_grad, upper_key, upper_value = attention(mask, queries, grad_out, kv, None)
    upstream = head_total(contract_last(query_grad, w_query[1]), cotangent)

    queries = jnp.dot(mid, w_query[0], preferred_element_type=F32).astype(BF16)
    grad_out = contract_last(upstream, w_out[0]).astype(BF16)
    query_grad, key_sum, value_sum = attention(
        mask, queries, grad_out, kv, (upper_key, upper_value)
    )
    kv_grad = lax.psum_scatter(
        jnp.concatenate([key_sum, value_sum], axis=1), "seq", scatter_dimension=0, tiled=True
    )
    w_kv = jnp.concatenate([w_key, w_value], axis=1)
    mid_part = contract_last(query_grad, w_query[0]) + contract_last(kv_grad, w_kv)
    grad_mid = head_total(mid_part, upstream)
    weight_part = contract_first(mid, kv_grad).astype(BF16)
    weight_grad = lax.psum(weight_part, "seq").astype(F32)
    grad_w_key, grad_w_value = weight_grad[:, :width], weight_grad[:, width:]

    grad_o = contract_last(grad_mid, w_ret_out).astype(BF16)
    grow, own_grad = grad_states(ret_query, grad_o, accum)
    device_grad = jnp.zeros_like(device_state)
    for block in reversed(range(count)):
        device_grad = own_grad[:, block] + decay_rows[:, block, None, None] * device_grad
    grads = gather_states(device_grad).reshape(peers, heads, E, E)
    outgoing = sum(c[:, None, None] * grads[k].astype(F32) for k, c in enumerate(backward))
    entering_list = []
    state_now = incoming
    for block in range(count):
        entering_list.append(state_now)
        state_now = decay_rows[:, block, None, None] * state_now + own_state[:, block]
    after_list = [state_now] * count
    state_now = outgoing
    for block in reversed(range(count)):
        after_list[block] = state_now
        state_now = own_grad[:, block] + decay_rows[:, block, None, None] * state_now
    entering = jnp.stack(entering_list, axis=1)
    after = jnp.stack(after_list, axis=1)
    grad_query, grad_key, grad_value = retention_grads(
        ret_query, ret_key, ret_value, grad_o, accum, shrink, grow, entering, after
    )
    return (grad_mid, grad_query, grad_key, grad_value, grad_w_key, grad_w_value)


def solution(mesh):
    placed = (
        P("seq", None),
        P("seq", None),
        P("seq", None),
        P(None, "head"),
        P(None, "head"),
        P(None, None, "head"),
        P(None, "head", None),
        P("head", None),
        P("seq", "head"),
        P("seq", "head"),
        P("seq", "head"),
        P("head", "seq"),
        P("head"),
        P("seq"),
    )
    return jax.shard_map(
        local,
        mesh=mesh,
        in_specs=placed,
        out_specs=(
            P("seq", None),
            P("seq", "head"),
            P("seq", "head"),
            P("seq", "head"),
            P(None, "head"),
            P(None, "head"),
        ),
        check_vma=False,
    )
```

```python
import functools
import math

import jax
import jax.numpy as jnp
from jax import lax
from jax.experimental import pallas as pl
from jax.experimental.pallas import tpu as pltpu
from jax.sharding import PartitionSpec as P

E = 128
BLK = 128
RC = 128
F32 = jnp.float32
BF16 = jnp.bfloat16


def contract_last(left, right):
    return lax.dot_general(left, right, (((1,), (1,)), ((), ())), preferred_element_type=F32)


def contract_first(left, right):
    return lax.dot_general(left, right, (((0,), (0,)), ((), ())), preferred_element_type=F32)


def send(src, dst, send_sem, recv_sem, axis, index):
    return pltpu.make_async_remote_copy(
        src_ref=src,
        dst_ref=dst,
        send_sem=send_sem,
        recv_sem=recv_sem,
        device_id={axis: index},
        device_id_type=pl.DeviceIdType.MESH,
    )


class SeqPlace:
    def __init__(self):
        self.peers = lax.axis_size("seq")
        self.chips = self.peers // 2
        self.me = lax.axis_index("seq")
        self.chip = self.me // 2
        self.core = lax.rem(self.me, 2)
        self.sibling = self.me + 1 - 2 * self.core

    def mate(self, k):
        return lax.rem(self.me + 2 * k, self.peers)

    def mate_of_sibling(self, k):
        return lax.rem(self.sibling + 2 * k, self.peers)


def rows_at(ref, index, rows):
    return ref.at[pl.ds(pl.multiple_of(index * rows, rows), rows)]


class Gather:
    def __init__(self, place, source, out, sems):
        self.place, self.source, self.out = place, source, out
        self.sends, self.forwards, self.arrivals = sems
        self.rows = out.shape[0] // place.peers

    @staticmethod
    def semaphores(peers):
        return [
            pltpu.SemaphoreType.DMA((peers // 2,)),
            pltpu.SemaphoreType.DMA((peers // 2,)),
            pltpu.SemaphoreType.DMA((peers,)),
        ]

    def chunk(self, index):
        return rows_at(self.out, index, self.rows)

    def direct(self, k):
        p = self.place
        return send(self.source, self.chunk(p.me), self.sends.at[k], self.arrivals.at[p.me], "seq", p.mate(k))

    def relayed(self, k):
        p = self.place
        at = p.mate(k)
        src = self.source if k == 0 else self.chunk(at)
        return send(src, self.chunk(at), self.forwards.at[k], self.arrivals.at[at], "seq", p.sibling)

    def arrival(self, index):
        p = self.place
        return send(self.source, self.chunk(index), self.sends.at[0], self.arrivals.at[index], "seq", p.sibling)

    def start(self):
        for k in range(1, self.place.chips):
            self.direct(k).start()
        self.relayed(0).start()

    def relay(self):
        for k in range(1, self.place.chips):
            self.arrival(self.place.mate(k)).wait_recv()
            self.relayed(k).start()

    def finish(self):
        p = self.place
        for k in range(p.chips):
            self.arrival(p.mate_of_sibling(k)).wait_recv()
        for k in range(1, p.chips):
            self.direct(k).wait_send()
        for k in range(p.chips):
            self.relayed(k).wait_send()


class Scatter:
    def __init__(self, place, source, scratch):
        self.place, self.source = place, source
        self.from_sibling, self.summed, self.landed = scratch[:3]
        self.pair_send, self.pair_recv, self.far_send, self.far_recv = scratch[3:]
        self.rows = source.shape[0] // place.peers

    @staticmethod
    def scratch(peers, rows, columns):
        chips = peers // 2
        return [
            pltpu.VMEM((chips, rows, columns), BF16),
            pltpu.VMEM((chips, rows, columns), BF16),
            pltpu.VMEM((chips, rows, columns), BF16),
        ] + [pltpu.SemaphoreType.DMA((chips,))] * 4

    def pair(self, i):
        p = self.place
        return send(
            rows_at(self.source, 2 * i + 1 - p.core, self.rows),
            self.from_sibling.at[i],
            self.pair_send.at[i],
            self.pair_recv.at[i],
            "seq",
            p.sibling,
        )

    def far(self, k):
        p = self.place
        return send(
            self.summed.at[k], self.landed.at[k], self.far_send.at[k], self.far_recv.at[k], "seq", p.mate(k)
        )

    def pair_total(self, i):
        p = self.place
        self.pair(i).wait_recv()
        own = self.source[pl.ds(pl.multiple_of((2 * i + p.core) * self.rows, self.rows), self.rows), :]
        return own.astype(F32) + self.from_sibling[i].astype(F32)

    def start(self):
        for k in range(self.place.chips):
            self.pair(lax.rem(self.place.chip + 1 + k, self.place.chips)).start()

    def combine(self):
        p = self.place
        for k in range(1, p.chips):
            self.summed[k] = self.pair_total(lax.rem(p.chip + k, p.chips)).astype(BF16)
            self.far(k).start()

    def total(self):
        p = self.place
        total = self.pair_total(p.chip)
        for k in range(1, p.chips):
            self.far(k).wait_recv()
            total = total + self.landed[k].astype(F32)
        return total.astype(BF16)

    def finish(self):
        for i in range(self.place.chips):
            self.pair(i).wait_send()
        for k in range(1, self.place.chips):
            self.far(k).wait_send()


CHUNK = 16


class HeadSum:
    def __init__(self, part, residual, out, scratch):
        self.part, self.residual, self.out = part, residual, out
        self.landed, self.summed = scratch[:2]
        self.up_send, self.up_recv, self.back_send, self.back_recv = scratch[2:]
        self.n = lax.axis_size("head")
        self.z = lax.axis_index("head")
        self.count = part.shape[0] // CHUNK
        self.half = part.shape[1] // 2
        self.steps = self.count + 3 * (self.n - 1)

    @staticmethod
    def scratch(rows, columns):
        sems = pltpu.SemaphoreType.DMA((2, rows // CHUNK))
        return [pltpu.VMEM((rows, columns), BF16)] * 2 + [sems] * 4

    def piece(self, half, j):
        return pl.ds(pl.multiple_of(j * CHUNK, CHUNK), CHUNK), pl.ds(half * self.half, self.half)

    def way(self, half):
        if half == 0:
            return self.z, self.z - 1, self.z + 1
        return self.n - 1 - self.z, self.z + 1, self.z - 1

    def up(self, half, j):
        at = self.piece(half, j)
        return send(
            self.summed.at[at], self.landed.at[at], self.up_send.at[half, j], self.up_recv.at[half, j],
            "head", self.way(half)[2],
        )

    def back(self, half, j):
        at = self.piece(half, j)
        return send(
            self.out.at[at], self.out.at[at], self.back_send.at[half, j], self.back_recv.at[half, j],
            "head", self.way(half)[1],
        )

    def add(self, half, j):
        place = self.way(half)[0]
        at = self.piece(half, j)

        @pl.when(place == 0)
        def _():
            self.summed[at] = self.part[at]
            self.up(half, j).start()

        @pl.when(place > 0)
        def _():
            self.up(half, j).wait_recv()
            total = self.part[at].astype(F32) + self.landed[at].astype(F32)

            @pl.when(place < self.n - 1)
            def _():
                self.summed[at] = total.astype(BF16)
                self.up(half, j).start()

            @pl.when(place == self.n - 1)
            def _():
                self.out[at] = (self.residual[at].astype(F32) + total).astype(BF16)
                self.back(half, j).start()

    def give_back(self, half, j):
        place = self.way(half)[0]

        @pl.when(place < self.n - 1)
        def _():
            self.back(half, j).wait_recv()

            @pl.when(place > 0)
            def _():
                self.back(half, j).start()

    def run(self, first, last):
        def step(t, carry):
            @pl.when(t < self.count)
            def _():
                self.add(0, t)
                self.add(1, t)

            for half in (0, 1):
                j = t - 3 * (self.n - 1 - self.way(half)[0])

                @pl.when((j >= 0) & (j < self.count))
                def _(half=half, j=j):
                    self.give_back(half, j)

            return carry

        lax.fori_loop(first, last, step, 0)

    def finish(self):
        def step(j, carry):
            for half in (0, 1):
                place = self.way(half)[0]

                @pl.when(place < self.n - 1)
                def _(half=half):
                    self.up(half, j).wait_send()

                @pl.when(place > 0)
                def _(half=half):
                    self.back(half, j).wait_send()

            return carry

        lax.fori_loop(0, self.count, step, 0)


def meet(seq, head):
    barrier = pltpu.get_barrier_semaphore()
    expected = 0

    def greet(axis, index):
        pl.semaphore_signal(
            barrier, inc=1, device_id={axis: index}, device_id_type=pl.DeviceIdType.MESH
        )

    if seq is not None:
        for k in range(1, seq.chips):
            greet("seq", seq.mate(k))
        greet("seq", seq.sibling)
        expected = seq.chips
    if head:
        n, z = lax.axis_size("head"), lax.axis_index("head")

        @pl.when(z > 0)
        def _():
            greet("head", z - 1)

        @pl.when(z < n - 1)
        def _():
            greet("head", z + 1)

        expected = expected + jnp.where(z > 0, 1, 0) + jnp.where(z < n - 1, 1, 0)
    pl.semaphore_wait(barrier, expected)


def call(kernel, name, number, outs, scratch, *operands):
    whole = pl.BlockSpec(memory_space=pltpu.VMEM)
    return pl.pallas_call(
        kernel,
        out_shape=outs,
        in_specs=[whole] * len(operands),
        out_specs=jax.tree.map(lambda _: whole, outs),
        scratch_shapes=scratch,
        compiler_params=pltpu.CompilerParams(
            collective_id=number, has_side_effects=True, vmem_limit_bytes=56 * 2**20
        ),
        name=name,
    )(*operands)


def gather_kernel(x_ref, out_ref, *sems):
    place = SeqPlace()
    meet(place, False)
    gather = Gather(place, x_ref, out_ref, sems)
    gather.start()
    out_ref[pl.ds(pl.multiple_of(place.me * gather.rows, gather.rows), gather.rows), :] = x_ref[...]
    gather.relay()
    gather.finish()


def gather_seq(x, name, number):
    peers = lax.axis_size("seq")
    out = jax.ShapeDtypeStruct((peers * x.shape[0], x.shape[1]), x.dtype)
    return call(gather_kernel, name, number, out, Gather.semaphores(peers), x)


def scatter_kernel(x_ref, out_ref, *scratch):
    place = SeqPlace()
    meet(place, False)
    scatter = Scatter(place, x_ref, scratch)
    scatter.start()
    scatter.combine()
    out_ref[...] = scatter.total()
    scatter.finish()


def scatter_seq(x, name, number):
    peers = lax.axis_size("seq")
    rows = x.shape[0] // peers
    out = jax.ShapeDtypeStruct((rows, x.shape[1]), BF16)
    return call(scatter_kernel, name, number, out, Scatter.scratch(peers, rows, x.shape[1]), x)


def first_sum_kernel(part, residual, state, decay, out, states, decays, *scratch):
    place = SeqPlace()
    meet(place, True)
    head = HeadSum(part, residual, out, scratch[:6])
    small = Gather(place, decay, decays, scratch[6:9])
    large = Gather(place, state, states, scratch[9:12])
    small.start()
    large.start()
    head.run(0, head.count)
    for gather, source in ((small, decay), (large, state)):
        gather.out[pl.ds(pl.multiple_of(place.me * gather.rows, gather.rows), gather.rows), :] = source[...]
        gather.relay()
    head.run(head.count, head.steps)
    small.finish()
    large.finish()
    head.finish()


def first_sum(part, residual, state, decay):
    peers = lax.axis_size("seq")
    outs = (
        jax.ShapeDtypeStruct(part.shape, BF16),
        jax.ShapeDtypeStruct((peers * state.shape[0], state.shape[1]), state.dtype),
        jax.ShapeDtypeStruct((peers * decay.shape[0], decay.shape[1]), decay.dtype),
    )
    scratch = HeadSum.scratch(*part.shape) + Gather.semaphores(peers) + Gather.semaphores(peers)
    return call(first_sum_kernel, "first_sum", 1, outs, scratch, part, residual, state, decay)


def second_sum_kernel(part, residual, weights, out, totals, *scratch):
    place = SeqPlace()
    meet(place, True)
    head = HeadSum(part, residual, out, scratch[:6])
    scatter = Scatter(place, weights, scratch[6:13])
    own = rows_at(totals, place.me, totals.shape[0] // place.peers)
    gather = Gather(place, own, totals, scratch[13:16])
    scatter.start()
    head.run(0, 2)
    scatter.combine()
    head.run(2, 12)
    own[...] = scatter.total()
    gather.start()
    head.run(12, head.steps - 2)
    gather.relay()
    head.run(head.steps - 2, head.steps)
    gather.finish()
    scatter.finish()
    head.finish()


def second_sum(part, residual, weights):
    peers = lax.axis_size("seq")
    outs = (
        jax.ShapeDtypeStruct(part.shape, BF16),
        jax.ShapeDtypeStruct(weights.shape, BF16),
    )
    scratch = (
        HeadSum.scratch(*part.shape)
        + Scatter.scratch(peers, weights.shape[0] // peers, weights.shape[1])
        + Gather.semaphores(peers)
    )
    return call(second_sum_kernel, "second_sum", 3, outs, scratch, part, residual, weights)


def attention_kernel(group, step, has_prev, mask_ref, *refs):
    if has_prev:
        q_ref, g_ref, k_ref, v_ref, pk_ref, pv_ref, dq_ref, dk_ref, dv_ref = refs[:9]
        s_ref, dk_acc, dv_acc = refs[9:]
    else:
        q_ref, g_ref, k_ref, v_ref, dq_ref, dk_ref, dv_ref, s_ref = refs
        dk_acc, dv_acc = dk_ref, dv_ref
    factor = 1.0 / math.sqrt(E)
    block = pl.program_id(1)
    first_row = mask_ref[0] + block * BLK
    first_key = mask_ref[1 + block]
    rows = group * BLK

    @pl.when(block == 0)
    def _():
        if has_prev:
            dk_acc[...] = pk_ref[...]
            dv_acc[...] = pv_ref[...]
        else:
            dk_acc[...] = jnp.zeros_like(dk_acc)
            dv_acc[...] = jnp.zeros_like(dv_acc)

    q = jnp.concatenate([q_ref[:, i * E : (i + 1) * E] for i in range(group)], axis=0)
    g = jnp.concatenate([g_ref[:, i * E : (i + 1) * E] for i in range(group)], axis=0)
    low = first_key // step
    high = (first_row + BLK + step - 1) // step
    query_position = first_row + lax.broadcasted_iota(jnp.int32, (BLK, step), 0)

    def span(j):
        return pl.ds(pl.multiple_of(j * step, step), step)

    def score(j, top):
        scores = contract_last(q, k_ref[span(j), :]) * factor
        at = j * step + lax.broadcasted_iota(jnp.int32, (BLK, step), 1)
        seen = (at >= first_key) & (at <= query_position)
        seen = jnp.concatenate([seen] * group, axis=0)
        scores = jnp.where(seen, scores, -jnp.inf)
        s_ref[:, span(j)] = scores
        return jnp.maximum(top, jnp.max(scores, axis=-1, keepdims=True))

    top = lax.fori_loop(low, high, score, jnp.full((rows, 1), -jnp.inf, F32))

    def raise_(j, total):
        raised = jnp.exp(s_ref[:, span(j)] - top)
        s_ref[:, span(j)] = raised
        return total + jnp.sum(raised, axis=-1, keepdims=True)

    total = lax.fori_loop(low, high, raise_, jnp.zeros((rows, 1), F32))
    scale = 1.0 / total

    def output(j, out):
        probs = s_ref[:, span(j)] * scale
        s_ref[:, span(j)] = probs
        return out + jnp.dot(probs.astype(BF16), v_ref[span(j), :], preferred_element_type=F32)

    out = lax.fori_loop(low, high, output, jnp.zeros((rows, E), F32)).astype(BF16)
    delta = jnp.sum(g.astype(F32) * out.astype(F32), axis=-1, keepdims=True)

    def back(j, dq):
        probs = s_ref[:, span(j)]
        dprobs = contract_last(g, v_ref[span(j), :])
        dscores = (probs * (dprobs - delta) * factor).astype(BF16)
        dk_acc[span(j), :] += contract_first(dscores, q)
        dv_acc[span(j), :] += contract_first(probs.astype(BF16), g)
        return dq + jnp.dot(dscores, k_ref[span(j), :], preferred_element_type=F32)

    dq = lax.fori_loop(low, high, back, jnp.zeros((rows, E), F32)).astype(BF16)
    for i in range(group):
        dq_ref[:, i * E : (i + 1) * E] = dq[i * BLK : (i + 1) * BLK, :]
    if has_prev:

        @pl.when(block == pl.num_programs(1) - 1)
        def _():
            dk_ref[...] = dk_acc[...].astype(BF16)
            dv_ref[...] = dv_acc[...].astype(BF16)


def attention(mask, queries, grad_out, kv, previous):
    row_count, width = queries.shape
    key_count, both = kv.shape
    heads = both // (2 * E)
    group = width // (heads * E)
    step = 256 if key_count % 256 == 0 else BLK
    has_prev = previous is not None
    tile = pl.BlockSpec((BLK, group * E), lambda h, b, m: (b, h))
    key_block = pl.BlockSpec((key_count, E), lambda h, b, m: (0, h))
    value_block = pl.BlockSpec((key_count, E), lambda h, b, m: (0, h + heads))
    part = jax.ShapeDtypeStruct((key_count, heads * E), BF16 if has_prev else F32)
    scratch = [pltpu.VMEM((group * BLK, key_count), F32)]
    if has_prev:
        scratch += [pltpu.VMEM((key_count, E), F32)] * 2
    return pl.pallas_call(
        functools.partial(attention_kernel, group, step, has_prev),
        out_shape=(jax.ShapeDtypeStruct((row_count, width), BF16), part, part),
        grid_spec=pltpu.PrefetchScalarGridSpec(
            num_scalar_prefetch=1,
            grid=(heads, row_count // BLK),
            in_specs=[tile, tile, key_block, value_block] + [key_block] * (2 if has_prev else 0),
            out_specs=(tile, key_block, key_block),
            scratch_shapes=scratch,
        ),
        compiler_params=pltpu.CompilerParams(vmem_limit_bytes=48 * 2**20),
        cost_estimate=pl.CostEstimate(
            flops=10 * row_count * width * key_count, bytes_accessed=8 * 2**20, transcendentals=0
        ),
        name="attention_back",
    )(mask, queries, grad_out, kv, kv, *(previous or ()))


def retention_states(ret_key, ret_value, gate, decay_exp):
    length, width = ret_key.shape
    heads = gate.shape[0]
    size = width // heads
    count = length // RC
    key_blocks = ret_key.reshape(count, RC, heads, size)
    value_blocks = ret_value.reshape(count, RC, heads, size)
    rate = jnp.exp2(-decay_exp.astype(F32) / 64.0)
    accum = jnp.cumsum((-rate[:, None] * gate).reshape(heads, count, RC), axis=2)
    ends = accum[:, :, -1]
    shrink = jnp.transpose(jnp.exp(ends[:, :, None] - accum), (1, 2, 0))[..., None]
    weighted = (shrink * key_blocks).astype(BF16)
    own_state = jnp.einsum("csha,cshb->hcab", weighted, value_blocks, preferred_element_type=F32)
    return (accum, ends, shrink, own_state)


def grad_states(ret_query, grad_o, accum):
    heads, count, block = accum.shape
    size = ret_query.shape[1] // heads
    query_blocks = ret_query.reshape(count, block, heads, size)
    grad_blocks = grad_o.reshape(count, block, heads, size)
    grow = jnp.transpose(jnp.exp(accum), (1, 2, 0))[..., None]
    weighted = (grow * query_blocks).astype(BF16)
    own_grad = jnp.einsum("ctha,cthb->hcab", weighted, grad_blocks, preferred_element_type=F32) / E
    return (grow, own_grad)


def retention_grads(ret_query, ret_key, ret_value, grad_o, accum, shrink, grow, entering, after):
    length, width = ret_query.shape
    heads, count, block = accum.shape
    size = width // heads
    shape4 = (count, block, heads, size)
    query_blocks = ret_query.reshape(shape4)
    key_blocks = ret_key.reshape(shape4)
    value_blocks = ret_value.reshape(shape4)
    grad_blocks = grad_o.reshape(shape4)
    lower = jnp.arange(block)[:, None] >= jnp.arange(block)[None, :]
    diff = accum[:, :, :, None] - accum[:, :, None, :]
    weights = jnp.where(lower, jnp.exp(jnp.where(lower, diff, 0.0)), 0.0)
    dot = functools.partial(jnp.einsum, preferred_element_type=F32)
    first = (weights * dot("ctha,csha->hcts", grad_blocks, value_blocks)).astype(BF16)
    second = (weights * dot("ctha,csha->hcts", query_blocks, key_blocks)).astype(BF16)
    inner_query = dot("hcts,csha->ctha", first, key_blocks)
    inner_key = dot("hcts,ctha->csha", first, query_blocks)
    inner_value = dot("hcts,ctha->csha", second, grad_blocks)
    entering = entering.astype(BF16)
    after = after.astype(BF16)
    carried_query = dot("cthb,hcab->ctha", grad_blocks, entering)
    carried_key = dot("cshb,hcab->csha", value_blocks, after)
    carried_value = dot("csha,hcab->cshb", key_blocks, after)
    grad_query = ((inner_query + grow * carried_query) / E).astype(BF16).reshape(length, width)
    grad_key = (inner_key / E + shrink * carried_key).astype(BF16).reshape(length, width)
    grad_value = (inner_value / E + shrink * carried_value).astype(BF16).reshape(length, width)
    return (grad_query, grad_key, grad_value)


def local(
    mid,
    second_in,
    cotangent,
    w_key,
    w_value,
    w_query,
    w_out,
    w_ret_out,
    ret_query,
    ret_key,
    ret_value,
    gate,
    decay_exp,
    mask_start,
):
    row_count = mid.shape[0]
    peers, position = lax.axis_size("seq"), lax.axis_index("seq")
    accum, ends, shrink, own_state = retention_states(ret_key, ret_value, gate, decay_exp)
    decay_rows = jnp.exp(ends)
    heads, count = decay_rows.shape
    device_decay = jnp.prod(decay_rows, axis=1)
    device_state = jnp.zeros_like(own_state[:, 0])
    for block in range(count):
        device_state = decay_rows[:, block, None, None] * device_state + own_state[:, block]
    kv_own = jnp.concatenate(
        [
            jnp.dot(mid, w_key, preferred_element_type=F32).astype(BF16),
            jnp.dot(mid, w_value, preferred_element_type=F32).astype(BF16),
        ],
        axis=1,
    )
    kv = gather_seq(kv_own, "gather_kv", 0)
    mask = jnp.concatenate([(position * row_count)[None].astype(jnp.int32), mask_start])
    width = w_key.shape[1]

    queries = jnp.dot(second_in, w_query[1], preferred_element_type=F32).astype(BF16)
    grad_out = contract_last(cotangent, w_out[1]).astype(BF16)
    query_grad, upper_key, upper_value = attention(mask, queries, grad_out, kv, None)
    upstream, states, decays = first_sum(
        contract_last(query_grad, w_query[1]).astype(BF16),
        cotangent,
        device_state.astype(BF16).reshape(heads * E, E),
        jnp.pad(device_decay[None, :], ((0, 7), (0, E - heads))),
    )
    states = states.reshape(peers, heads, E, E)
    decays = decays.reshape(peers, 8, E)[:, 0, :heads]
    forward, backward = [], []
    for k in range(peers):
        pf = jnp.where(k < position, 1.0, 0.0) * jnp.ones((heads,), F32)
        pb = jnp.where(k > position, 1.0, 0.0) * jnp.ones((heads,), F32)
        for m in range(peers):
            if m > k:
                pf = pf * jnp.where(m < position, decays[m], 1.0)
            if m < k:
                pb = pb * jnp.where(m > position, decays[m], 1.0)
        forward.append(pf)
        backward.append(pb)
    incoming = sum(c[:, None, None] * states[k].astype(F32) for k, c in enumerate(forward))

    queries = jnp.dot(mid, w_query[0], preferred_element_type=F32).astype(BF16)
    grad_out = contract_last(upstream, w_out[0]).astype(BF16)
    query_grad, key_sum, value_sum = attention(
        mask, queries, grad_out, kv, (upper_key, upper_value)
    )
    kv_grad = scatter_seq(jnp.concatenate([key_sum, value_sum], axis=1), "scatter_kv", 2)
    w_kv = jnp.concatenate([w_key, w_value], axis=1)
    mid_part = contract_last(query_grad, w_query[0]) + contract_last(kv_grad, w_kv)
    grad_mid, weight_grad = second_sum(
        mid_part.astype(BF16), upstream, contract_first(mid, kv_grad).astype(BF16)
    )
    weight_grad = weight_grad.astype(F32)
    grad_w_key, grad_w_value = weight_grad[:, :width], weight_grad[:, width:]

    grad_o = contract_last(grad_mid, w_ret_out).astype(BF16)
    grow, own_grad = grad_states(ret_query, grad_o, accum)
    device_grad = jnp.zeros_like(device_state)
    for block in reversed(range(count)):
        device_grad = own_grad[:, block] + decay_rows[:, block, None, None] * device_grad
    grads = gather_seq(device_grad.astype(BF16).reshape(heads * E, E), "gather_grads", 4)
    grads = grads.reshape(peers, heads, E, E)
    outgoing = sum(c[:, None, None] * grads[k].astype(F32) for k, c in enumerate(backward))
    entering_list = []
    state_now = incoming
    for block in range(count):
        entering_list.append(state_now)
        state_now = decay_rows[:, block, None, None] * state_now + own_state[:, block]
    after_list = [state_now] * count
    state_now = outgoing
    for block in reversed(range(count)):
        after_list[block] = state_now
        state_now = own_grad[:, block] + decay_rows[:, block, None, None] * state_now
    entering = jnp.stack(entering_list, axis=1)
    after = jnp.stack(after_list, axis=1)
    grad_query, grad_key, grad_value = retention_grads(
        ret_query, ret_key, ret_value, grad_o, accum, shrink, grow, entering, after
    )
    return (grad_mid, grad_query, grad_key, grad_value, grad_w_key, grad_w_value)


def solution(mesh):
    placed = (
        P("seq", None),
        P("seq", None),
        P("seq", None),
        P(None, "head"),
        P(None, "head"),
        P(None, None, "head"),
        P(None, "head", None),
        P("head", None),
        P("seq", "head"),
        P("seq", "head"),
        P("seq", "head"),
        P("head", "seq"),
        P("head"),
        P("seq"),
    )
    return jax.shard_map(
        local,
        mesh=mesh,
        in_specs=placed,
        out_specs=(
            P("seq", None),
            P("seq", "head"),
            P("seq", "head"),
            P("seq", "head"),
            P(None, "head"),
            P(None, "head"),
        ),
        check_vma=False,
    )
```

```python
import functools
import math

import jax
import jax.numpy as jnp
from jax import lax
from jax.experimental import pallas as pl
from jax.experimental.pallas import tpu as pltpu
from jax.sharding import PartitionSpec as P

E = 128
BLK = 128
RC = 128
F32 = jnp.float32
BF16 = jnp.bfloat16


def contract_last(left, right):
    return lax.dot_general(left, right, (((1,), (1,)), ((), ())), preferred_element_type=F32)


def contract_first(left, right):
    return lax.dot_general(left, right, (((0,), (0,)), ((), ())), preferred_element_type=F32)


def send(src, dst, send_sem, recv_sem, axis, index):
    return pltpu.make_async_remote_copy(
        src_ref=src,
        dst_ref=dst,
        send_sem=send_sem,
        recv_sem=recv_sem,
        device_id={axis: index},
        device_id_type=pl.DeviceIdType.MESH,
    )


class SeqPlace:
    def __init__(self):
        self.peers = lax.axis_size("seq")
        self.chips = self.peers // 2
        self.me = lax.axis_index("seq")
        self.chip = self.me // 2
        self.core = lax.rem(self.me, 2)
        self.sibling = self.me + 1 - 2 * self.core

    def mate(self, k):
        return lax.rem(self.me + 2 * k, self.peers)

    def mate_of_sibling(self, k):
        return lax.rem(self.sibling + 2 * k, self.peers)


def rows_at(ref, index, rows):
    return ref.at[pl.ds(pl.multiple_of(index * rows, rows), rows)]


class Gather:
    def __init__(self, place, source, out, sems):
        self.place, self.source, self.out = place, source, out
        self.sends, self.forwards, self.arrivals = sems
        self.rows = out.shape[0] // place.peers

    @staticmethod
    def semaphores(peers):
        return [
            pltpu.SemaphoreType.DMA((peers // 2,)),
            pltpu.SemaphoreType.DMA((peers // 2,)),
            pltpu.SemaphoreType.DMA((peers,)),
        ]

    def chunk(self, index):
        return rows_at(self.out, index, self.rows)

    def direct(self, k):
        p = self.place
        return send(self.source, self.chunk(p.me), self.sends.at[k], self.arrivals.at[p.me], "seq", p.mate(k))

    def relayed(self, k):
        p = self.place
        at = p.mate(k)
        src = self.source if k == 0 else self.chunk(at)
        return send(src, self.chunk(at), self.forwards.at[k], self.arrivals.at[at], "seq", p.sibling)

    def arrival(self, index):
        p = self.place
        return send(self.source, self.chunk(index), self.sends.at[0], self.arrivals.at[index], "seq", p.sibling)

    def start(self):
        for k in range(1, self.place.chips):
            self.direct(k).start()
        self.relayed(0).start()

    def relay(self):
        for k in range(1, self.place.chips):
            self.arrival(self.place.mate(k)).wait_recv()
            self.relayed(k).start()

    def finish(self):
        p = self.place
        for k in range(p.chips):
            self.arrival(p.mate_of_sibling(k)).wait_recv()
        for k in range(1, p.chips):
            self.direct(k).wait_send()
        for k in range(p.chips):
            self.relayed(k).wait_send()


class Scatter:
    def __init__(self, place, source, scratch):
        self.place, self.source = place, source
        self.from_sibling, self.summed, self.landed = scratch[:3]
        self.pair_send, self.pair_recv, self.far_send, self.far_recv = scratch[3:]
        self.rows = source.shape[0] // place.peers

    @staticmethod
    def scratch(peers, rows, columns):
        chips = peers // 2
        return [
            pltpu.VMEM((chips, rows, columns), BF16),
            pltpu.VMEM((chips, rows, columns), BF16),
            pltpu.VMEM((chips, rows, columns), BF16),
        ] + [pltpu.SemaphoreType.DMA((chips,))] * 4

    def pair(self, i):
        p = self.place
        return send(
            rows_at(self.source, 2 * i + 1 - p.core, self.rows),
            self.from_sibling.at[i],
            self.pair_send.at[i],
            self.pair_recv.at[i],
            "seq",
            p.sibling,
        )

    def far(self, k):
        p = self.place
        return send(
            self.summed.at[k], self.landed.at[k], self.far_send.at[k], self.far_recv.at[k], "seq", p.mate(k)
        )

    def pair_total(self, i):
        p = self.place
        self.pair(i).wait_recv()
        own = self.source[pl.ds(pl.multiple_of((2 * i + p.core) * self.rows, self.rows), self.rows), :]
        return own.astype(F32) + self.from_sibling[i].astype(F32)

    def start(self):
        for k in range(self.place.chips):
            self.pair(lax.rem(self.place.chip + 1 + k, self.place.chips)).start()

    def combine(self):
        p = self.place
        for k in range(1, p.chips):
            self.summed[k] = self.pair_total(lax.rem(p.chip + k, p.chips)).astype(BF16)
            self.far(k).start()

    def total(self):
        p = self.place
        total = self.pair_total(p.chip)
        for k in range(1, p.chips):
            self.far(k).wait_recv()
            total = total + self.landed[k].astype(F32)
        return total.astype(BF16)

    def finish(self):
        for i in range(self.place.chips):
            self.pair(i).wait_send()
        for k in range(1, self.place.chips):
            self.far(k).wait_send()


CHUNK = 16
LAG = 2


class HeadSum:
    def __init__(self, part, residual, out, scratch):
        self.part, self.residual, self.out = part, residual, out
        self.landed, self.summed = scratch[:2]
        self.up_send, self.up_recv, self.back_send, self.back_recv = scratch[2:]
        self.n = lax.axis_size("head")
        self.z = lax.axis_index("head")
        self.count = part.shape[0] // CHUNK
        self.half = part.shape[1] // 2
        self.steps = self.count + 2 * LAG * (self.n - 1)

    @staticmethod
    def scratch(rows, columns):
        sems = pltpu.SemaphoreType.DMA((2, rows // CHUNK))
        return [pltpu.VMEM((rows, columns), BF16)] * 2 + [sems] * 4

    def piece(self, half, j):
        return pl.ds(pl.multiple_of(j * CHUNK, CHUNK), CHUNK), pl.ds(half * self.half, self.half)

    def way(self, half):
        if half == 0:
            return self.z, self.z - 1, self.z + 1
        return self.n - 1 - self.z, self.z + 1, self.z - 1

    def up(self, half, j):
        at = self.piece(half, j)
        return send(
            self.summed.at[at], self.landed.at[at], self.up_send.at[half, j], self.up_recv.at[half, j],
            "head", self.way(half)[2],
        )

    def back(self, half, j):
        at = self.piece(half, j)
        return send(
            self.out.at[at], self.out.at[at], self.back_send.at[half, j], self.back_recv.at[half, j],
            "head", self.way(half)[1],
        )

    def add(self, half, j):
        place = self.way(half)[0]
        at = self.piece(half, j)

        @pl.when(place == 0)
        def _():
            self.summed[at] = self.part[at]
            self.up(half, j).start()

        @pl.when(place > 0)
        def _():
            self.up(half, j).wait_recv()
            total = self.part[at].astype(F32) + self.landed[at].astype(F32)

            @pl.when(place < self.n - 1)
            def _():
                self.summed[at] = total.astype(BF16)
                self.up(half, j).start()

            @pl.when(place == self.n - 1)
            def _():
                self.out[at] = (self.residual[at].astype(F32) + total).astype(BF16)
                self.back(half, j).start()

    def give_back(self, half, j):
        place = self.way(half)[0]

        @pl.when(place < self.n - 1)
        def _():
            self.back(half, j).wait_recv()

            @pl.when(place > 0)
            def _():
                self.back(half, j).start()

    def run(self, first, last):
        def step(t, carry):
            for half in (0, 1):
                place = self.way(half)[0]
                up = t - LAG * place
                down = t - LAG * (2 * (self.n - 1) - place)

                @pl.when((up >= 0) & (up < self.count))
                def _(half=half, up=up):
                    self.add(half, up)

                @pl.when((down >= 0) & (down < self.count))
                def _(half=half, down=down):
                    self.give_back(half, down)

            return carry

        lax.fori_loop(first, last, step, 0)

    def finish(self):
        def step(j, carry):
            for half in (0, 1):
                place = self.way(half)[0]

                @pl.when(place < self.n - 1)
                def _(half=half):
                    self.up(half, j).wait_send()

                @pl.when(place > 0)
                def _(half=half):
                    self.back(half, j).wait_send()

            return carry

        lax.fori_loop(0, self.count, step, 0)


def meet(seq, head):
    barrier = pltpu.get_barrier_semaphore()
    expected = 0

    def greet(axis, index):
        pl.semaphore_signal(
            barrier, inc=1, device_id={axis: index}, device_id_type=pl.DeviceIdType.MESH
        )

    if seq is not None:
        for k in range(1, seq.chips):
            greet("seq", seq.mate(k))
        greet("seq", seq.sibling)
        expected = seq.chips
    if head:
        n, z = lax.axis_size("head"), lax.axis_index("head")

        @pl.when(z > 0)
        def _():
            greet("head", z - 1)

        @pl.when(z < n - 1)
        def _():
            greet("head", z + 1)

        expected = expected + jnp.where(z > 0, 1, 0) + jnp.where(z < n - 1, 1, 0)
    pl.semaphore_wait(barrier, expected)


def call(kernel, name, number, outs, scratch, *operands):
    whole = pl.BlockSpec(memory_space=pltpu.VMEM)
    return pl.pallas_call(
        kernel,
        out_shape=outs,
        in_specs=[whole] * len(operands),
        out_specs=jax.tree.map(lambda _: whole, outs),
        scratch_shapes=scratch,
        compiler_params=pltpu.CompilerParams(
            collective_id=number, has_side_effects=True, vmem_limit_bytes=56 * 2**20
        ),
        name=name,
    )(*operands)


def gather_kernel(x_ref, out_ref, *sems):
    place = SeqPlace()
    meet(place, False)
    gather = Gather(place, x_ref, out_ref, sems)
    gather.start()
    out_ref[pl.ds(pl.multiple_of(place.me * gather.rows, gather.rows), gather.rows), :] = x_ref[...]
    gather.relay()
    gather.finish()


def gather_seq(x, name, number):
    peers = lax.axis_size("seq")
    out = jax.ShapeDtypeStruct((peers * x.shape[0], x.shape[1]), x.dtype)
    return call(gather_kernel, name, number, out, Gather.semaphores(peers), x)


def scatter_kernel(x_ref, out_ref, *scratch):
    place = SeqPlace()
    meet(place, False)
    scatter = Scatter(place, x_ref, scratch)
    scatter.start()
    scatter.combine()
    out_ref[...] = scatter.total()
    scatter.finish()


def scatter_seq(x, name, number):
    peers = lax.axis_size("seq")
    rows = x.shape[0] // peers
    out = jax.ShapeDtypeStruct((rows, x.shape[1]), BF16)
    return call(scatter_kernel, name, number, out, Scatter.scratch(peers, rows, x.shape[1]), x)


def first_sum_kernel(part, residual, state, decay, out, states, decays, *scratch):
    place = SeqPlace()
    meet(place, True)
    head = HeadSum(part, residual, out, scratch[:6])
    small = Gather(place, decay, decays, scratch[6:9])
    large = Gather(place, state, states, scratch[9:12])
    small.start()
    large.start()
    head.run(0, head.count)
    for gather, source in ((small, decay), (large, state)):
        gather.out[pl.ds(pl.multiple_of(place.me * gather.rows, gather.rows), gather.rows), :] = source[...]
        gather.relay()
    head.run(head.count, head.steps)
    small.finish()
    large.finish()
    head.finish()


def first_sum(part, residual, state, decay):
    peers = lax.axis_size("seq")
    outs = (
        jax.ShapeDtypeStruct(part.shape, BF16),
        jax.ShapeDtypeStruct((peers * state.shape[0], state.shape[1]), state.dtype),
        jax.ShapeDtypeStruct((peers * decay.shape[0], decay.shape[1]), decay.dtype),
    )
    scratch = HeadSum.scratch(*part.shape) + Gather.semaphores(peers) + Gather.semaphores(peers)
    return call(first_sum_kernel, "first_sum", 1, outs, scratch, part, residual, state, decay)


def second_sum_kernel(part, residual, weights, out, totals, *scratch):
    place = SeqPlace()
    meet(place, True)
    head = HeadSum(part, residual, out, scratch[:6])
    scatter = Scatter(place, weights, scratch[6:13])
    own = rows_at(totals, place.me, totals.shape[0] // place.peers)
    gather = Gather(place, own, totals, scratch[13:16])
    scatter.start()
    head.run(0, 2)
    scatter.combine()
    head.run(2, 12)
    own[...] = scatter.total()
    gather.start()
    head.run(12, head.steps - 2)
    gather.relay()
    head.run(head.steps - 2, head.steps)
    gather.finish()
    scatter.finish()
    head.finish()


def second_sum(part, residual, weights):
    peers = lax.axis_size("seq")
    outs = (
        jax.ShapeDtypeStruct(part.shape, BF16),
        jax.ShapeDtypeStruct(weights.shape, BF16),
    )
    scratch = (
        HeadSum.scratch(*part.shape)
        + Scatter.scratch(peers, weights.shape[0] // peers, weights.shape[1])
        + Gather.semaphores(peers)
    )
    return call(second_sum_kernel, "second_sum", 3, outs, scratch, part, residual, weights)


def attention_kernel(group, step, has_prev, mask_ref, *refs):
    if has_prev:
        q_ref, g_ref, k_ref, v_ref, pk_ref, pv_ref, dq_ref, dk_ref, dv_ref = refs[:9]
        s_ref, dk_acc, dv_acc = refs[9:]
    else:
        q_ref, g_ref, k_ref, v_ref, dq_ref, dk_ref, dv_ref, s_ref = refs
        dk_acc, dv_acc = dk_ref, dv_ref
    factor = 1.0 / math.sqrt(E)
    block = pl.program_id(1)
    first_row = mask_ref[0] + block * BLK
    first_key = mask_ref[1 + block]
    rows = group * BLK

    @pl.when(block == 0)
    def _():
        if has_prev:
            dk_acc[...] = pk_ref[...]
            dv_acc[...] = pv_ref[...]
        else:
            dk_acc[...] = jnp.zeros_like(dk_acc)
            dv_acc[...] = jnp.zeros_like(dv_acc)

    q = jnp.concatenate([q_ref[:, i * E : (i + 1) * E] for i in range(group)], axis=0)
    g = jnp.concatenate([g_ref[:, i * E : (i + 1) * E] for i in range(group)], axis=0)
    low = first_key // step
    high = (first_row + BLK + step - 1) // step
    query_position = first_row + lax.broadcasted_iota(jnp.int32, (BLK, step), 0)

    def span(j):
        return pl.ds(pl.multiple_of(j * step, step), step)

    def score(j, top):
        scores = contract_last(q, k_ref[span(j), :]) * factor
        at = j * step + lax.broadcasted_iota(jnp.int32, (BLK, step), 1)
        seen = (at >= first_key) & (at <= query_position)
        seen = jnp.concatenate([seen] * group, axis=0)
        scores = jnp.where(seen, scores, -jnp.inf)
        s_ref[:, span(j)] = scores
        return jnp.maximum(top, jnp.max(scores, axis=-1, keepdims=True))

    top = lax.fori_loop(low, high, score, jnp.full((rows, 1), -jnp.inf, F32))

    def raise_(j, total):
        raised = jnp.exp(s_ref[:, span(j)] - top)
        s_ref[:, span(j)] = raised
        return total + jnp.sum(raised, axis=-1, keepdims=True)

    total = lax.fori_loop(low, high, raise_, jnp.zeros((rows, 1), F32))
    scale = 1.0 / total

    def output(j, out):
        probs = s_ref[:, span(j)] * scale
        s_ref[:, span(j)] = probs
        return out + jnp.dot(probs.astype(BF16), v_ref[span(j), :], preferred_element_type=F32)

    out = lax.fori_loop(low, high, output, jnp.zeros((rows, E), F32)).astype(BF16)
    delta = jnp.sum(g.astype(F32) * out.astype(F32), axis=-1, keepdims=True)

    def back(j, dq):
        probs = s_ref[:, span(j)]
        dprobs = contract_last(g, v_ref[span(j), :])
        dscores = (probs * (dprobs - delta) * factor).astype(BF16)
        dk_acc[span(j), :] += contract_first(dscores, q)
        dv_acc[span(j), :] += contract_first(probs.astype(BF16), g)
        return dq + jnp.dot(dscores, k_ref[span(j), :], preferred_element_type=F32)

    dq = lax.fori_loop(low, high, back, jnp.zeros((rows, E), F32)).astype(BF16)
    for i in range(group):
        dq_ref[:, i * E : (i + 1) * E] = dq[i * BLK : (i + 1) * BLK, :]
    if has_prev:

        @pl.when(block == pl.num_programs(1) - 1)
        def _():
            dk_ref[...] = dk_acc[...].astype(BF16)
            dv_ref[...] = dv_acc[...].astype(BF16)


def attention(mask, queries, grad_out, kv, previous):
    row_count, width = queries.shape
    key_count, both = kv.shape
    heads = both // (2 * E)
    group = width // (heads * E)
    step = 256 if key_count % 256 == 0 else BLK
    has_prev = previous is not None
    tile = pl.BlockSpec((BLK, group * E), lambda h, b, m: (b, h))
    key_block = pl.BlockSpec((key_count, E), lambda h, b, m: (0, h))
    value_block = pl.BlockSpec((key_count, E), lambda h, b, m: (0, h + heads))
    part = jax.ShapeDtypeStruct((key_count, heads * E), BF16 if has_prev else F32)
    scratch = [pltpu.VMEM((group * BLK, key_count), F32)]
    if has_prev:
        scratch += [pltpu.VMEM((key_count, E), F32)] * 2
    return pl.pallas_call(
        functools.partial(attention_kernel, group, step, has_prev),
        out_shape=(jax.ShapeDtypeStruct((row_count, width), BF16), part, part),
        grid_spec=pltpu.PrefetchScalarGridSpec(
            num_scalar_prefetch=1,
            grid=(heads, row_count // BLK),
            in_specs=[tile, tile, key_block, value_block] + [key_block] * (2 if has_prev else 0),
            out_specs=(tile, key_block, key_block),
            scratch_shapes=scratch,
        ),
        compiler_params=pltpu.CompilerParams(vmem_limit_bytes=48 * 2**20),
        cost_estimate=pl.CostEstimate(
            flops=10 * row_count * width * key_count, bytes_accessed=8 * 2**20, transcendentals=0
        ),
        name="attention_back",
    )(mask, queries, grad_out, kv, kv, *(previous or ()))


def retention_states(ret_key, ret_value, gate, decay_exp):
    length, width = ret_key.shape
    heads = gate.shape[0]
    size = width // heads
    count = length // RC
    key_blocks = ret_key.reshape(count, RC, heads, size)
    value_blocks = ret_value.reshape(count, RC, heads, size)
    rate = jnp.exp2(-decay_exp.astype(F32) / 64.0)
    accum = jnp.cumsum((-rate[:, None] * gate).reshape(heads, count, RC), axis=2)
    ends = accum[:, :, -1]
    shrink = jnp.transpose(jnp.exp(ends[:, :, None] - accum), (1, 2, 0))[..., None]
    weighted = (shrink * key_blocks).astype(BF16)
    own_state = jnp.einsum("csha,cshb->hcab", weighted, value_blocks, preferred_element_type=F32)
    return (accum, ends, shrink, own_state)


def grad_states(ret_query, grad_o, accum):
    heads, count, block = accum.shape
    size = ret_query.shape[1] // heads
    query_blocks = ret_query.reshape(count, block, heads, size)
    grad_blocks = grad_o.reshape(count, block, heads, size)
    grow = jnp.transpose(jnp.exp(accum), (1, 2, 0))[..., None]
    weighted = (grow * query_blocks).astype(BF16)
    own_grad = jnp.einsum("ctha,cthb->hcab", weighted, grad_blocks, preferred_element_type=F32) / E
    return (grow, own_grad)


def retention_grads(ret_query, ret_key, ret_value, grad_o, accum, shrink, grow, entering, after):
    length, width = ret_query.shape
    heads, count, block = accum.shape
    size = width // heads
    shape4 = (count, block, heads, size)
    query_blocks = ret_query.reshape(shape4)
    key_blocks = ret_key.reshape(shape4)
    value_blocks = ret_value.reshape(shape4)
    grad_blocks = grad_o.reshape(shape4)
    lower = jnp.arange(block)[:, None] >= jnp.arange(block)[None, :]
    diff = accum[:, :, :, None] - accum[:, :, None, :]
    weights = jnp.where(lower, jnp.exp(jnp.where(lower, diff, 0.0)), 0.0)
    dot = functools.partial(jnp.einsum, preferred_element_type=F32)
    first = (weights * dot("ctha,csha->hcts", grad_blocks, value_blocks)).astype(BF16)
    second = (weights * dot("ctha,csha->hcts", query_blocks, key_blocks)).astype(BF16)
    inner_query = dot("hcts,csha->ctha", first, key_blocks)
    inner_key = dot("hcts,ctha->csha", first, query_blocks)
    inner_value = dot("hcts,ctha->csha", second, grad_blocks)
    entering = entering.astype(BF16)
    after = after.astype(BF16)
    carried_query = dot("cthb,hcab->ctha", grad_blocks, entering)
    carried_key = dot("cshb,hcab->csha", value_blocks, after)
    carried_value = dot("csha,hcab->cshb", key_blocks, after)
    grad_query = ((inner_query + grow * carried_query) / E).astype(BF16).reshape(length, width)
    grad_key = (inner_key / E + shrink * carried_key).astype(BF16).reshape(length, width)
    grad_value = (inner_value / E + shrink * carried_value).astype(BF16).reshape(length, width)
    return (grad_query, grad_key, grad_value)


def local(
    mid,
    second_in,
    cotangent,
    w_key,
    w_value,
    w_query,
    w_out,
    w_ret_out,
    ret_query,
    ret_key,
    ret_value,
    gate,
    decay_exp,
    mask_start,
):
    row_count = mid.shape[0]
    peers, position = lax.axis_size("seq"), lax.axis_index("seq")
    accum, ends, shrink, own_state = retention_states(ret_key, ret_value, gate, decay_exp)
    decay_rows = jnp.exp(ends)
    heads, count = decay_rows.shape
    device_decay = jnp.prod(decay_rows, axis=1)
    device_state = jnp.zeros_like(own_state[:, 0])
    for block in range(count):
        device_state = decay_rows[:, block, None, None] * device_state + own_state[:, block]
    kv_own = jnp.concatenate(
        [
            jnp.dot(mid, w_key, preferred_element_type=F32).astype(BF16),
            jnp.dot(mid, w_value, preferred_element_type=F32).astype(BF16),
        ],
        axis=1,
    )
    kv = gather_seq(kv_own, "gather_kv", 0)
    mask = jnp.concatenate([(position * row_count)[None].astype(jnp.int32), mask_start])
    width = w_key.shape[1]

    queries = jnp.dot(second_in, w_query[1], preferred_element_type=F32).astype(BF16)
    grad_out = contract_last(cotangent, w_out[1]).astype(BF16)
    query_grad, upper_key, upper_value = attention(mask, queries, grad_out, kv, None)
    upstream, states, decays = first_sum(
        contract_last(query_grad, w_query[1]).astype(BF16),
        cotangent,
        device_state.astype(BF16).reshape(heads * E, E),
        jnp.pad(device_decay[None, :], ((0, 7), (0, E - heads))),
    )
    states = states.reshape(peers, heads, E, E)
    decays = decays.reshape(peers, 8, E)[:, 0, :heads]
    forward, backward = [], []
    for k in range(peers):
        pf = jnp.where(k < position, 1.0, 0.0) * jnp.ones((heads,), F32)
        pb = jnp.where(k > position, 1.0, 0.0) * jnp.ones((heads,), F32)
        for m in range(peers):
            if m > k:
                pf = pf * jnp.where(m < position, decays[m], 1.0)
            if m < k:
                pb = pb * jnp.where(m > position, decays[m], 1.0)
        forward.append(pf)
        backward.append(pb)
    incoming = sum(c[:, None, None] * states[k].astype(F32) for k, c in enumerate(forward))

    queries = jnp.dot(mid, w_query[0], preferred_element_type=F32).astype(BF16)
    grad_out = contract_last(upstream, w_out[0]).astype(BF16)
    query_grad, key_sum, value_sum = attention(
        mask, queries, grad_out, kv, (upper_key, upper_value)
    )
    kv_grad = scatter_seq(jnp.concatenate([key_sum, value_sum], axis=1), "scatter_kv", 2)
    w_kv = jnp.concatenate([w_key, w_value], axis=1)
    mid_part = contract_last(query_grad, w_query[0]) + contract_last(kv_grad, w_kv)
    grad_mid, weight_grad = second_sum(
        mid_part.astype(BF16), upstream, contract_first(mid, kv_grad).astype(BF16)
    )
    weight_grad = weight_grad.astype(F32)
    grad_w_key, grad_w_value = weight_grad[:, :width], weight_grad[:, width:]

    grad_o = contract_last(grad_mid, w_ret_out).astype(BF16)
    grow, own_grad = grad_states(ret_query, grad_o, accum)
    device_grad = jnp.zeros_like(device_state)
    for block in reversed(range(count)):
        device_grad = own_grad[:, block] + decay_rows[:, block, None, None] * device_grad
    grads = gather_seq(device_grad.astype(BF16).reshape(heads * E, E), "gather_grads", 4)
    grads = grads.reshape(peers, heads, E, E)
    outgoing = sum(c[:, None, None] * grads[k].astype(F32) for k, c in enumerate(backward))
    entering_list = []
    state_now = incoming
    for block in range(count):
        entering_list.append(state_now)
        state_now = decay_rows[:, block, None, None] * state_now + own_state[:, block]
    after_list = [state_now] * count
    state_now = outgoing
    for block in reversed(range(count)):
        after_list[block] = state_now
        state_now = own_grad[:, block] + decay_rows[:, block, None, None] * state_now
    entering = jnp.stack(entering_list, axis=1)
    after = jnp.stack(after_list, axis=1)
    grad_query, grad_key, grad_value = retention_grads(
        ret_query, ret_key, ret_value, grad_o, accum, shrink, grow, entering, after
    )
    return (grad_mid, grad_query, grad_key, grad_value, grad_w_key, grad_w_value)


def solution(mesh):
    placed = (
        P("seq", None),
        P("seq", None),
        P("seq", None),
        P(None, "head"),
        P(None, "head"),
        P(None, None, "head"),
        P(None, "head", None),
        P("head", None),
        P("seq", "head"),
        P("seq", "head"),
        P("seq", "head"),
        P("head", "seq"),
        P("head"),
        P("seq"),
    )
    return jax.shard_map(
        local,
        mesh=mesh,
        in_specs=placed,
        out_specs=(
            P("seq", None),
            P("seq", "head"),
            P("seq", "head"),
            P("seq", "head"),
            P(None, "head"),
            P(None, "head"),
        ),
        check_vma=False,
    )
```

```python
import functools
import math

import jax
import jax.numpy as jnp
from jax import lax
from jax.experimental import pallas as pl
from jax.experimental.pallas import tpu as pltpu
from jax.sharding import PartitionSpec as P

E = 128
BLK = 128
RC = 128
F32 = jnp.float32
BF16 = jnp.bfloat16


def contract_last(left, right):
    return lax.dot_general(left, right, (((1,), (1,)), ((), ())), preferred_element_type=F32)


def contract_first(left, right):
    return lax.dot_general(left, right, (((0,), (0,)), ((), ())), preferred_element_type=F32)


def send(src, dst, send_sem, recv_sem, axis, index):
    return pltpu.make_async_remote_copy(
        src_ref=src,
        dst_ref=dst,
        send_sem=send_sem,
        recv_sem=recv_sem,
        device_id={axis: index},
        device_id_type=pl.DeviceIdType.MESH,
    )


class SeqPlace:
    def __init__(self):
        self.peers = lax.axis_size("seq")
        self.chips = self.peers // 2
        self.me = lax.axis_index("seq")
        self.chip = self.me // 2
        self.core = lax.rem(self.me, 2)
        self.sibling = self.me + 1 - 2 * self.core

    def mate(self, k):
        return lax.rem(self.me + 2 * k, self.peers)

    def mate_of_sibling(self, k):
        return lax.rem(self.sibling + 2 * k, self.peers)


def rows_at(ref, index, rows):
    return ref.at[pl.ds(pl.multiple_of(index * rows, rows), rows)]


class Gather:
    def __init__(self, place, source, out, sems):
        self.place, self.source, self.out = place, source, out
        self.sends, self.forwards, self.arrivals = sems
        self.rows = out.shape[0] // place.peers

    @staticmethod
    def semaphores(peers):
        return [
            pltpu.SemaphoreType.DMA((peers // 2,)),
            pltpu.SemaphoreType.DMA((peers // 2,)),
            pltpu.SemaphoreType.DMA((peers,)),
        ]

    def chunk(self, index):
        return rows_at(self.out, index, self.rows)

    def direct(self, k):
        p = self.place
        return send(self.source, self.chunk(p.me), self.sends.at[k], self.arrivals.at[p.me], "seq", p.mate(k))

    def relayed(self, k):
        p = self.place
        at = p.mate(k)
        src = self.source if k == 0 else self.chunk(at)
        return send(src, self.chunk(at), self.forwards.at[k], self.arrivals.at[at], "seq", p.sibling)

    def arrival(self, index):
        p = self.place
        return send(self.source, self.chunk(index), self.sends.at[0], self.arrivals.at[index], "seq", p.sibling)

    def start(self):
        for k in range(1, self.place.chips):
            self.direct(k).start()
        self.relayed(0).start()

    def relay(self):
        for k in range(1, self.place.chips):
            self.arrival(self.place.mate(k)).wait_recv()
            self.relayed(k).start()

    def finish(self):
        p = self.place
        for k in range(p.chips):
            self.arrival(p.mate_of_sibling(k)).wait_recv()
        for k in range(1, p.chips):
            self.direct(k).wait_send()
        for k in range(p.chips):
            self.relayed(k).wait_send()


class Scatter:
    def __init__(self, place, source, scratch):
        self.place, self.source = place, source
        self.from_sibling, self.summed, self.landed = scratch[:3]
        self.pair_send, self.pair_recv, self.far_send, self.far_recv = scratch[3:]
        self.rows = source.shape[0] // place.peers

    @staticmethod
    def scratch(peers, rows, columns):
        chips = peers // 2
        return [
            pltpu.VMEM((chips, rows, columns), BF16),
            pltpu.VMEM((chips, rows, columns), BF16),
            pltpu.VMEM((chips, rows, columns), BF16),
        ] + [pltpu.SemaphoreType.DMA((chips,))] * 4

    def pair(self, i):
        p = self.place
        return send(
            rows_at(self.source, 2 * i + 1 - p.core, self.rows),
            self.from_sibling.at[i],
            self.pair_send.at[i],
            self.pair_recv.at[i],
            "seq",
            p.sibling,
        )

    def far(self, k):
        p = self.place
        return send(
            self.summed.at[k], self.landed.at[k], self.far_send.at[k], self.far_recv.at[k], "seq", p.mate(k)
        )

    def pair_total(self, i):
        p = self.place
        self.pair(i).wait_recv()
        own = self.source[pl.ds(pl.multiple_of((2 * i + p.core) * self.rows, self.rows), self.rows), :]
        return own.astype(F32) + self.from_sibling[i].astype(F32)

    def start(self):
        for k in range(self.place.chips):
            self.pair(lax.rem(self.place.chip + 1 + k, self.place.chips)).start()

    def combine(self):
        p = self.place
        for k in range(1, p.chips):
            self.summed[k] = self.pair_total(lax.rem(p.chip + k, p.chips)).astype(BF16)
            self.far(k).start()

    def total(self):
        p = self.place
        total = self.pair_total(p.chip)
        for k in range(1, p.chips):
            self.far(k).wait_recv()
            total = total + self.landed[k].astype(F32)
        return total.astype(BF16)

    def finish(self):
        for i in range(self.place.chips):
            self.pair(i).wait_send()
        for k in range(1, self.place.chips):
            self.far(k).wait_send()


CHUNK = 16
LAG = 3


class HeadSum:
    def __init__(self, part, residual, out, scratch):
        self.part, self.residual, self.out = part, residual, out
        self.landed, self.summed = scratch[:2]
        self.up_send, self.up_recv, self.back_send, self.back_recv = scratch[2:]
        self.n = lax.axis_size("head")
        self.z = lax.axis_index("head")
        self.count = part.shape[0] // CHUNK
        self.half = part.shape[1] // 2
        self.steps = self.count + 2 * LAG * (self.n - 1)

    @staticmethod
    def scratch(rows, columns):
        sems = pltpu.SemaphoreType.DMA((2, rows // CHUNK))
        return [pltpu.VMEM((rows, columns), BF16)] * 2 + [sems] * 4

    def piece(self, half, j):
        return pl.ds(pl.multiple_of(j * CHUNK, CHUNK), CHUNK), pl.ds(half * self.half, self.half)

    def way(self, half):
        if half == 0:
            return self.z, self.z - 1, self.z + 1
        return self.n - 1 - self.z, self.z + 1, self.z - 1

    def up(self, half, j):
        at = self.piece(half, j)
        return send(
            self.summed.at[at], self.landed.at[at], self.up_send.at[half, j], self.up_recv.at[half, j],
            "head", self.way(half)[2],
        )

    def back(self, half, j):
        at = self.piece(half, j)
        return send(
            self.out.at[at], self.out.at[at], self.back_send.at[half, j], self.back_recv.at[half, j],
            "head", self.way(half)[1],
        )

    def add(self, half, j):
        place = self.way(half)[0]
        at = self.piece(half, j)

        @pl.when(place == 0)
        def _():
            self.summed[at] = self.part[at]
            self.up(half, j).start()

        @pl.when(place > 0)
        def _():
            self.up(half, j).wait_recv()
            total = self.part[at].astype(F32) + self.landed[at].astype(F32)

            @pl.when(place < self.n - 1)
            def _():
                self.summed[at] = total.astype(BF16)
                self.up(half, j).start()

            @pl.when(place == self.n - 1)
            def _():
                self.out[at] = (self.residual[at].astype(F32) + total).astype(BF16)
                self.back(half, j).start()

    def give_back(self, half, j):
        place = self.way(half)[0]

        @pl.when(place < self.n - 1)
        def _():
            self.back(half, j).wait_recv()

            @pl.when(place > 0)
            def _():
                self.back(half, j).start()

    def run(self, first, last):
        def step(t, carry):
            for half in (0, 1):
                place = self.way(half)[0]
                up = t - LAG * place
                down = t - LAG * (2 * (self.n - 1) - place)

                @pl.when((up >= 0) & (up < self.count))
                def _(half=half, up=up):
                    self.add(half, up)

                @pl.when((down >= 0) & (down < self.count))
                def _(half=half, down=down):
                    self.give_back(half, down)

            return carry

        lax.fori_loop(first, last, step, 0)

    def finish(self):
        def step(j, carry):
            for half in (0, 1):
                place = self.way(half)[0]

                @pl.when(place < self.n - 1)
                def _(half=half):
                    self.up(half, j).wait_send()

                @pl.when(place > 0)
                def _(half=half):
                    self.back(half, j).wait_send()

            return carry

        lax.fori_loop(0, self.count, step, 0)


def meet(seq, head):
    barrier = pltpu.get_barrier_semaphore()
    expected = 0

    def greet(axis, index):
        pl.semaphore_signal(
            barrier, inc=1, device_id={axis: index}, device_id_type=pl.DeviceIdType.MESH
        )

    if seq is not None:
        for k in range(1, seq.chips):
            greet("seq", seq.mate(k))
        greet("seq", seq.sibling)
        expected = seq.chips
    if head:
        n, z = lax.axis_size("head"), lax.axis_index("head")

        @pl.when(z > 0)
        def _():
            greet("head", z - 1)

        @pl.when(z < n - 1)
        def _():
            greet("head", z + 1)

        expected = expected + jnp.where(z > 0, 1, 0) + jnp.where(z < n - 1, 1, 0)
    pl.semaphore_wait(barrier, expected)


def call(kernel, name, number, outs, scratch, *operands, far=0):
    whole = pl.BlockSpec(memory_space=pltpu.VMEM)
    return pl.pallas_call(
        kernel,
        out_shape=outs,
        in_specs=[whole] * (len(operands) - far) + [pl.BlockSpec(memory_space=pl.ANY)] * far,
        out_specs=jax.tree.map(lambda _: whole, outs),
        scratch_shapes=scratch,
        compiler_params=pltpu.CompilerParams(
            collective_id=number, has_side_effects=True, vmem_limit_bytes=56 * 2**20
        ),
        name=name,
    )(*operands)


def gather_kernel(x_ref, out_ref, *sems):
    place = SeqPlace()
    meet(place, False)
    gather = Gather(place, x_ref, out_ref, sems)
    gather.start()
    out_ref[pl.ds(pl.multiple_of(place.me * gather.rows, gather.rows), gather.rows), :] = x_ref[...]
    gather.relay()
    gather.finish()


def gather_seq(x, name, number):
    peers = lax.axis_size("seq")
    out = jax.ShapeDtypeStruct((peers * x.shape[0], x.shape[1]), x.dtype)
    return call(gather_kernel, name, number, out, Gather.semaphores(peers), x)


def tile_of(width):
    return 256 if width % 256 == 0 else E


def gather_project_kernel(
    x_ref, second_ref, cotangent_ref, mid_ref, wq_ref, wo_ref,
    out_ref, q1_ref, g1_ref, q0_ref,
    columns, rows, column_sem, row_sem, *sems
):
    place = SeqPlace()
    width = q1_ref.shape[1]
    tile = tile_of(width)
    pieces = width // tile

    def column_copy(layer, i):
        return pltpu.make_async_copy(
            wq_ref.at[layer, :, pl.ds(i * tile, tile)], columns.at[layer, i], column_sem.at[layer, i]
        )

    def row_copy(i):
        return pltpu.make_async_copy(wo_ref.at[1, pl.ds(i * tile, tile), :], rows.at[i], row_sem.at[i])

    for i in range(pieces):
        column_copy(1, i).start()
    for i in range(pieces):
        row_copy(i).start()
    for i in range(pieces):
        column_copy(0, i).start()
    meet(place, False)
    gather = Gather(place, x_ref, out_ref, sems)
    gather.start()
    out_ref[pl.ds(pl.multiple_of(place.me * gather.rows, gather.rows), gather.rows), :] = x_ref[...]
    for i in range(pieces):
        column_copy(1, i).wait()
        q1_ref[:, i * tile : (i + 1) * tile] = jnp.dot(
            second_ref[...], columns[1, i], preferred_element_type=F32
        ).astype(BF16)
    for i in range(pieces):
        row_copy(i).wait()
        g1_ref[:, i * tile : (i + 1) * tile] = contract_last(cotangent_ref[...], rows[i]).astype(BF16)
    gather.relay()
    for i in range(pieces):
        column_copy(0, i).wait()
        q0_ref[:, i * tile : (i + 1) * tile] = jnp.dot(
            mid_ref[...], columns[0, i], preferred_element_type=F32
        ).astype(BF16)
    gather.finish()


def gather_project(x, second_in, cotangent, mid, w_query, w_out):
    peers = lax.axis_size("seq")
    depth, width = w_query.shape[1:]
    tile = tile_of(width)
    pieces = width // tile
    projected = jax.ShapeDtypeStruct((mid.shape[0], width), BF16)
    outs = (jax.ShapeDtypeStruct((peers * x.shape[0], x.shape[1]), x.dtype),) + (projected,) * 3
    scratch = [
        pltpu.VMEM((2, pieces, depth, tile), BF16),
        pltpu.VMEM((pieces, tile, depth), BF16),
        pltpu.SemaphoreType.DMA((2, pieces)),
        pltpu.SemaphoreType.DMA((pieces,)),
    ] + Gather.semaphores(peers)
    return call(
        gather_project_kernel, "gather_kv", 0, outs, scratch,
        x, second_in, cotangent, mid, w_query, w_out, far=2,
    )


def scatter_project_kernel(x_ref, g_ref, wq_ref, out_ref, part_ref, slab, slab_sem, *scratch):
    place = SeqPlace()
    depth = part_ref.shape[1]
    pieces = slab.shape[0]
    size = depth // pieces

    def copy(i):
        return pltpu.make_async_copy(wq_ref.at[0, pl.ds(i * size, size), :], slab.at[i], slab_sem.at[i])

    for i in range(pieces):
        copy(i).start()
    meet(place, False)
    scatter = Scatter(place, x_ref, scratch)
    scatter.start()
    scatter.combine()
    for i in range(pieces):
        copy(i).wait()
        part_ref[:, i * size : (i + 1) * size] = contract_last(g_ref[...], slab[i])
    out_ref[...] = scatter.total()
    scatter.finish()


def scatter_project(x, query_grad, w_query):
    peers = lax.axis_size("seq")
    rows = x.shape[0] // peers
    depth, width = w_query.shape[1:]
    pieces = 6 if depth % (6 * E) == 0 else 1
    outs = (
        jax.ShapeDtypeStruct((rows, x.shape[1]), BF16),
        jax.ShapeDtypeStruct((query_grad.shape[0], depth), F32),
    )
    scratch = [
        pltpu.VMEM((pieces, depth // pieces, width), BF16),
        pltpu.SemaphoreType.DMA((pieces,)),
    ] + Scatter.scratch(peers, rows, x.shape[1])
    return call(scatter_project_kernel, "scatter_kv", 2, outs, scratch, x, query_grad, w_query, far=1)


def first_sum_kernel(part, residual, state, decay, out, states, decays, *scratch):
    place = SeqPlace()
    meet(place, True)
    head = HeadSum(part, residual, out, scratch[:6])
    small = Gather(place, decay, decays, scratch[6:9])
    large = Gather(place, state, states, scratch[9:12])
    small.start()
    large.start()
    head.run(0, head.count)
    for gather, source in ((small, decay), (large, state)):
        gather.out[pl.ds(pl.multiple_of(place.me * gather.rows, gather.rows), gather.rows), :] = source[...]
        gather.relay()
    head.run(head.count, head.steps)
    small.finish()
    large.finish()
    head.finish()


def first_sum(part, residual, state, decay):
    peers = lax.axis_size("seq")
    outs = (
        jax.ShapeDtypeStruct(part.shape, BF16),
        jax.ShapeDtypeStruct((peers * state.shape[0], state.shape[1]), state.dtype),
        jax.ShapeDtypeStruct((peers * decay.shape[0], decay.shape[1]), decay.dtype),
    )
    scratch = HeadSum.scratch(*part.shape) + Gather.semaphores(peers) + Gather.semaphores(peers)
    return call(first_sum_kernel, "first_sum", 1, outs, scratch, part, residual, state, decay)


def second_sum_kernel(part, residual, weights, out, totals, *scratch):
    place = SeqPlace()
    meet(place, True)
    head = HeadSum(part, residual, out, scratch[:6])
    scatter = Scatter(place, weights, scratch[6:13])
    own = rows_at(totals, place.me, totals.shape[0] // place.peers)
    gather = Gather(place, own, totals, scratch[13:16])
    scatter.start()
    head.run(0, 2)
    scatter.combine()
    head.run(2, 12)
    own[...] = scatter.total()
    gather.start()
    head.run(12, head.steps - 2)
    gather.relay()
    head.run(head.steps - 2, head.steps)
    gather.finish()
    scatter.finish()
    head.finish()


def second_sum(part, residual, weights):
    peers = lax.axis_size("seq")
    outs = (
        jax.ShapeDtypeStruct(part.shape, BF16),
        jax.ShapeDtypeStruct(weights.shape, BF16),
    )
    scratch = (
        HeadSum.scratch(*part.shape)
        + Scatter.scratch(peers, weights.shape[0] // peers, weights.shape[1])
        + Gather.semaphores(peers)
    )
    return call(second_sum_kernel, "second_sum", 3, outs, scratch, part, residual, weights)


def attention_kernel(group, step, has_prev, mask_ref, *refs):
    if has_prev:
        q_ref, g_ref, k_ref, v_ref, pk_ref, pv_ref, dq_ref, dk_ref, dv_ref = refs[:9]
        s_ref, dk_acc, dv_acc = refs[9:]
    else:
        q_ref, g_ref, k_ref, v_ref, dq_ref, dk_ref, dv_ref, s_ref = refs
        dk_acc, dv_acc = dk_ref, dv_ref
    factor = 1.0 / math.sqrt(E)
    block = pl.program_id(1)
    first_row = mask_ref[0] + block * BLK
    first_key = mask_ref[1 + block]
    rows = group * BLK

    @pl.when(block == 0)
    def _():
        if has_prev:
            dk_acc[...] = pk_ref[...]
            dv_acc[...] = pv_ref[...]
        else:
            dk_acc[...] = jnp.zeros_like(dk_acc)
            dv_acc[...] = jnp.zeros_like(dv_acc)

    q = jnp.concatenate([q_ref[:, i * E : (i + 1) * E] for i in range(group)], axis=0)
    g = jnp.concatenate([g_ref[:, i * E : (i + 1) * E] for i in range(group)], axis=0)
    low = first_key // step
    high = (first_row + BLK + step - 1) // step
    query_position = first_row + lax.broadcasted_iota(jnp.int32, (BLK, step), 0)

    def span(j):
        return pl.ds(pl.multiple_of(j * step, step), step)

    def score(j, top):
        scores = contract_last(q, k_ref[span(j), :]) * factor
        at = j * step + lax.broadcasted_iota(jnp.int32, (BLK, step), 1)
        seen = (at >= first_key) & (at <= query_position)
        seen = jnp.concatenate([seen] * group, axis=0)
        scores = jnp.where(seen, scores, -jnp.inf)
        s_ref[:, span(j)] = scores
        return jnp.maximum(top, jnp.max(scores, axis=-1, keepdims=True))

    top = lax.fori_loop(low, high, score, jnp.full((rows, 1), -jnp.inf, F32))

    def raise_(j, total):
        raised = jnp.exp(s_ref[:, span(j)] - top)
        s_ref[:, span(j)] = raised
        return total + jnp.sum(raised, axis=-1, keepdims=True)

    total = lax.fori_loop(low, high, raise_, jnp.zeros((rows, 1), F32))
    scale = 1.0 / total

    def output(j, out):
        probs = s_ref[:, span(j)] * scale
        s_ref[:, span(j)] = probs
        return out + jnp.dot(probs.astype(BF16), v_ref[span(j), :], preferred_element_type=F32)

    out = lax.fori_loop(low, high, output, jnp.zeros((rows, E), F32)).astype(BF16)
    delta = jnp.sum(g.astype(F32) * out.astype(F32), axis=-1, keepdims=True)

    def back(j, dq):
        probs = s_ref[:, span(j)]
        dprobs = contract_last(g, v_ref[span(j), :])
        dscores = (probs * (dprobs - delta) * factor).astype(BF16)
        dk_acc[span(j), :] += contract_first(dscores, q)
        dv_acc[span(j), :] += contract_first(probs.astype(BF16), g)
        return dq + jnp.dot(dscores, k_ref[span(j), :], preferred_element_type=F32)

    dq = lax.fori_loop(low, high, back, jnp.zeros((rows, E), F32)).astype(BF16)
    for i in range(group):
        dq_ref[:, i * E : (i + 1) * E] = dq[i * BLK : (i + 1) * BLK, :]
    if has_prev:

        @pl.when(block == pl.num_programs(1) - 1)
        def _():
            dk_ref[...] = dk_acc[...].astype(BF16)
            dv_ref[...] = dv_acc[...].astype(BF16)


def attention(mask, queries, grad_out, kv, previous):
    row_count, width = queries.shape
    key_count, both = kv.shape
    heads = both // (2 * E)
    group = width // (heads * E)
    step = 256 if key_count % 256 == 0 else BLK
    has_prev = previous is not None
    tile = pl.BlockSpec((BLK, group * E), lambda h, b, m: (b, h))
    key_block = pl.BlockSpec((key_count, E), lambda h, b, m: (0, h))
    value_block = pl.BlockSpec((key_count, E), lambda h, b, m: (0, h + heads))
    part = jax.ShapeDtypeStruct((key_count, heads * E), BF16 if has_prev else F32)
    scratch = [pltpu.VMEM((group * BLK, key_count), F32)]
    if has_prev:
        scratch += [pltpu.VMEM((key_count, E), F32)] * 2
    return pl.pallas_call(
        functools.partial(attention_kernel, group, step, has_prev),
        out_shape=(jax.ShapeDtypeStruct((row_count, width), BF16), part, part),
        grid_spec=pltpu.PrefetchScalarGridSpec(
            num_scalar_prefetch=1,
            grid=(heads, row_count // BLK),
            in_specs=[tile, tile, key_block, value_block] + [key_block] * (2 if has_prev else 0),
            out_specs=(tile, key_block, key_block),
            scratch_shapes=scratch,
        ),
        compiler_params=pltpu.CompilerParams(vmem_limit_bytes=48 * 2**20),
        cost_estimate=pl.CostEstimate(
            flops=10 * row_count * width * key_count, bytes_accessed=8 * 2**20, transcendentals=0
        ),
        name="attention_back",
    )(mask, queries, grad_out, kv, kv, *(previous or ()))


def retention_states(ret_key, ret_value, gate, decay_exp):
    length, width = ret_key.shape
    heads = gate.shape[0]
    size = width // heads
    count = length // RC
    key_blocks = ret_key.reshape(count, RC, heads, size)
    value_blocks = ret_value.reshape(count, RC, heads, size)
    rate = jnp.exp2(-decay_exp.astype(F32) / 64.0)
    accum = jnp.cumsum((-rate[:, None] * gate).reshape(heads, count, RC), axis=2)
    ends = accum[:, :, -1]
    shrink = jnp.transpose(jnp.exp(ends[:, :, None] - accum), (1, 2, 0))[..., None]
    weighted = (shrink * key_blocks).astype(BF16)
    own_state = jnp.einsum("csha,cshb->hcab", weighted, value_blocks, preferred_element_type=F32)
    return (accum, ends, shrink, own_state)


def grad_states(ret_query, grad_o, accum):
    heads, count, block = accum.shape
    size = ret_query.shape[1] // heads
    query_blocks = ret_query.reshape(count, block, heads, size)
    grad_blocks = grad_o.reshape(count, block, heads, size)
    grow = jnp.transpose(jnp.exp(accum), (1, 2, 0))[..., None]
    weighted = (grow * query_blocks).astype(BF16)
    own_grad = jnp.einsum("ctha,cthb->hcab", weighted, grad_blocks, preferred_element_type=F32) / E
    return (grow, own_grad)


def retention_grads(ret_query, ret_key, ret_value, grad_o, accum, shrink, grow, entering, after):
    length, width = ret_query.shape
    heads, count, block = accum.shape
    size = width // heads
    shape4 = (count, block, heads, size)
    query_blocks = ret_query.reshape(shape4)
    key_blocks = ret_key.reshape(shape4)
    value_blocks = ret_value.reshape(shape4)
    grad_blocks = grad_o.reshape(shape4)
    lower = jnp.arange(block)[:, None] >= jnp.arange(block)[None, :]
    diff = accum[:, :, :, None] - accum[:, :, None, :]
    weights = jnp.where(lower, jnp.exp(jnp.where(lower, diff, 0.0)), 0.0)
    dot = functools.partial(jnp.einsum, preferred_element_type=F32)
    first = (weights * dot("ctha,csha->hcts", grad_blocks, value_blocks)).astype(BF16)
    second = (weights * dot("ctha,csha->hcts", query_blocks, key_blocks)).astype(BF16)
    inner_query = dot("hcts,csha->ctha", first, key_blocks)
    inner_key = dot("hcts,ctha->csha", first, query_blocks)
    inner_value = dot("hcts,ctha->csha", second, grad_blocks)
    entering = entering.astype(BF16)
    after = after.astype(BF16)
    carried_query = dot("cthb,hcab->ctha", grad_blocks, entering)
    carried_key = dot("cshb,hcab->csha", value_blocks, after)
    carried_value = dot("csha,hcab->cshb", key_blocks, after)
    grad_query = ((inner_query + grow * carried_query) / E).astype(BF16).reshape(length, width)
    grad_key = (inner_key / E + shrink * carried_key).astype(BF16).reshape(length, width)
    grad_value = (inner_value / E + shrink * carried_value).astype(BF16).reshape(length, width)
    return (grad_query, grad_key, grad_value)


def local(
    mid,
    second_in,
    cotangent,
    w_key,
    w_value,
    w_query,
    w_out,
    w_ret_out,
    ret_query,
    ret_key,
    ret_value,
    gate,
    decay_exp,
    mask_start,
):
    row_count = mid.shape[0]
    peers, position = lax.axis_size("seq"), lax.axis_index("seq")
    accum, ends, shrink, own_state = retention_states(ret_key, ret_value, gate, decay_exp)
    decay_rows = jnp.exp(ends)
    heads, count = decay_rows.shape
    device_decay = jnp.sum(ends, axis=1)
    device_state = jnp.zeros_like(own_state[:, 0])
    for block in range(count):
        device_state = decay_rows[:, block, None, None] * device_state + own_state[:, block]
    kv_own = jnp.concatenate(
        [
            jnp.dot(mid, w_key, preferred_element_type=F32).astype(BF16),
            jnp.dot(mid, w_value, preferred_element_type=F32).astype(BF16),
        ],
        axis=1,
    )
    kv, queries, grad_out, lower_queries = gather_project(
        kv_own, second_in, cotangent, mid, w_query, w_out
    )
    mask = jnp.concatenate([(position * row_count)[None].astype(jnp.int32), mask_start])
    width = w_key.shape[1]

    query_grad, upper_key, upper_value = attention(mask, queries, grad_out, kv, None)
    upstream, states, decays = first_sum(
        contract_last(query_grad, w_query[1]).astype(BF16),
        cotangent,
        device_state.astype(BF16).reshape(heads * E, E),
        jnp.pad(device_decay[None, :], ((0, 7), (0, E - heads))),
    )
    states = states.reshape(peers, heads, E, E)
    decays = decays.reshape(peers, 8, E)[:, 0, :heads]
    source, between = jnp.arange(peers)[:, None, None], jnp.arange(peers)[None, :, None]
    logs = decays[None]
    ahead = jnp.sum(jnp.where((between > source) & (between < position), logs, 0.0), axis=1)
    behind = jnp.sum(jnp.where((between < source) & (between > position), logs, 0.0), axis=1)
    forward = jnp.where(source[:, 0] < position, jnp.exp(ahead), 0.0)
    backward = jnp.where(source[:, 0] > position, jnp.exp(behind), 0.0)
    incoming = jnp.sum(forward[:, :, None, None] * states.astype(F32), axis=0)

    grad_out = contract_last(upstream, w_out[0]).astype(BF16)
    query_grad, key_sum, value_sum = attention(
        mask, lower_queries, grad_out, kv, (upper_key, upper_value)
    )
    kv_grad, lower_in = scatter_project(
        jnp.concatenate([key_sum, value_sum], axis=1), query_grad, w_query
    )
    w_kv = jnp.concatenate([w_key, w_value], axis=1)
    mid_part = lower_in + contract_last(kv_grad, w_kv)
    grad_mid, weight_grad = second_sum(
        mid_part.astype(BF16), upstream, contract_first(mid, kv_grad).astype(BF16)
    )
    weight_grad = weight_grad.astype(F32)
    grad_w_key, grad_w_value = weight_grad[:, :width], weight_grad[:, width:]

    grad_o = contract_last(grad_mid, w_ret_out).astype(BF16)
    grow, own_grad = grad_states(ret_query, grad_o, accum)
    device_grad = jnp.zeros_like(device_state)
    for block in reversed(range(count)):
        device_grad = own_grad[:, block] + decay_rows[:, block, None, None] * device_grad
    grads = gather_seq(device_grad.astype(BF16).reshape(heads * E, E), "gather_grads", 4)
    grads = grads.reshape(peers, heads, E, E)
    outgoing = jnp.sum(backward[:, :, None, None] * grads.astype(F32), axis=0)
    entering_list = []
    state_now = incoming
    for block in range(count):
        entering_list.append(state_now)
        state_now = decay_rows[:, block, None, None] * state_now + own_state[:, block]
    after_list = [state_now] * count
    state_now = outgoing
    for block in reversed(range(count)):
        after_list[block] = state_now
        state_now = own_grad[:, block] + decay_rows[:, block, None, None] * state_now
    entering = jnp.stack(entering_list, axis=1)
    after = jnp.stack(after_list, axis=1)
    grad_query, grad_key, grad_value = retention_grads(
        ret_query, ret_key, ret_value, grad_o, accum, shrink, grow, entering, after
    )
    return (grad_mid, grad_query, grad_key, grad_value, grad_w_key, grad_w_value)


def solution(mesh):
    placed = (
        P("seq", None),
        P("seq", None),
        P("seq", None),
        P(None, "head"),
        P(None, "head"),
        P(None, None, "head"),
        P(None, "head", None),
        P("head", None),
        P("seq", "head"),
        P("seq", "head"),
        P("seq", "head"),
        P("head", "seq"),
        P("head"),
        P("seq"),
    )
    return jax.shard_map(
        local,
        mesh=mesh,
        in_specs=placed,
        out_specs=(
            P("seq", None),
            P("seq", "head"),
            P("seq", "head"),
            P("seq", "head"),
            P(None, "head"),
            P(None, "head"),
        ),
        check_vma=False,
    )
```
